128 devices in a mesh: heads: 1, cp: 128 (over z, y, x, core).
Axes of the slice: x: 4, y: 4, z: 4, core: 2. Of those that a mesh axis runs over, the one named last changes fastest.
Arguments:
- queries: bfloat16 [1, 2048, 56, 128], P(None, 'cp', 'heads')
- key_vecs: bfloat16 [6144, 56, 128], P('cp', 'heads')
- value_vecs: bfloat16 [6144, 56, 128], P('cp', 'heads')
- attn_out: bfloat16 [1, 2048, 56, 128], P(None, 'cp', 'heads')
- log_sum_exp: float32 [1, 2048, 56], P(None, 'cp', 'heads')
- grad_out: bfloat16 [1, 2048, 56, 128], P(None, 'cp', 'heads')
Outputs:
- output 1: bfloat16 [1, 2048, 56, 128], P(None, 'cp', 'heads')
- output 2: float32 [6144, 56, 128], P('cp', 'heads')
- output 3: float32 [6144, 56, 128], P('cp', 'heads')
All inputs are finite; a program needn't handle non-finite values.
Results may differ from the reference program's by a relative error of at most 0.00279.
Values are sent between devices in bfloat16 or wider.
A program may use at most 1 GiB of HBM per device.

```python
import jax
import jax.numpy as jnp
from jax import lax

SEGMENTS = 1
BLOCKS = 128
SEG_BLOCK = 16
KEY_BLOCK = 48
HEADS_PART = 56
HEAD_DIM = 128

SEG_LEN = BLOCKS * SEG_BLOCK
PREFIX = BLOCKS * KEY_BLOCK
PREFIX0 = PREFIX - SEGMENTS * SEG_LEN
N_QBLOCKS = SEGMENTS * BLOCKS
SCORE_SCALE = HEAD_DIM ** -0.5


def forward_all(queries, key_vecs, value_vecs):
    tile_shape = (BLOCKS, KEY_BLOCK, HEADS_PART, HEAD_DIM)
    key_tiles = key_vecs.astype(jnp.float32).reshape(tile_shape)
    value_tiles = value_vecs.astype(jnp.float32).reshape(tile_shape)
    tile_starts = KEY_BLOCK * jnp.arange(BLOCKS)
    q_blocks = queries.astype(jnp.float32).reshape(N_QBLOCKS, SEG_BLOCK, HEADS_PART, HEAD_DIM)
    q_starts = PREFIX0 + SEG_BLOCK * jnp.arange(N_QBLOCKS)

    def one_block(block_in):
        q_blk, q_start = block_in
        q_pos = q_start + jnp.arange(SEG_BLOCK)

        def key_step(state_in, tile_in):
            run_max, run_sum, acc_out = state_in
            k_tile, v_tile, k_start = tile_in
            k_pos = k_start + jnp.arange(KEY_BLOCK)
            causal = (q_pos[:, None] >= k_pos[None, :])[None]
            scores = jnp.einsum("qhd,khd->hqk", q_blk, k_tile) * SCORE_SCALE
            scores = jnp.where(causal, scores, -1e30)
            new_max = jnp.maximum(run_max, jnp.max(scores, axis=-1))
            rescale = jnp.exp(run_max - new_max)
            weights = jnp.exp(scores - new_max[:, :, None])
            run_sum = run_sum * rescale + jnp.sum(weights, axis=-1)
            acc_out = acc_out * rescale[:, :, None] + jnp.einsum("hqk,khd->hqd", weights, v_tile)
            return (new_max, run_sum, acc_out), None

        init_state = (jnp.full((HEADS_PART, SEG_BLOCK), -1e30, jnp.float32), jnp.zeros((HEADS_PART, SEG_BLOCK), jnp.float32), jnp.zeros((HEADS_PART, SEG_BLOCK, HEAD_DIM), jnp.float32))
        final_state, unused_ys = lax.scan(key_step, init_state, (key_tiles, value_tiles, tile_starts))
        run_max, run_sum, acc_out = final_state
        out_blk = jnp.transpose(acc_out / run_sum[:, :, None], (1, 0, 2))
        lse_blk = (run_max + jnp.log(run_sum)).T
        return out_blk, lse_blk

    out_blocks, lse_blocks = lax.map(one_block, (q_blocks, q_starts))
    return out_blocks.reshape(SEGMENTS, SEG_LEN, HEADS_PART, HEAD_DIM), lse_blocks.reshape(SEGMENTS, SEG_LEN, HEADS_PART)


def setup_inputs(seed: int = 0, part: int = 0) -> dict:
    base_key = jax.random.fold_in(jax.random.key(seed), part)
    key_q, key_k, key_v, key_mean, key_do = jax.random.split(base_key, 5)
    q_shape = (SEGMENTS, SEG_LEN, HEADS_PART, HEAD_DIM)
    kv_shape = (PREFIX, HEADS_PART, HEAD_DIM)
    queries = (1.5 * jax.random.normal(key_q, q_shape, jnp.float32)).astype(jnp.bfloat16)
    key_vecs = jax.random.normal(key_k, kv_shape, jnp.float32).astype(jnp.bfloat16)
    value_mean = jax.random.normal(key_mean, (1, HEADS_PART, HEAD_DIM), jnp.float32)
    value_vecs = (jax.random.normal(key_v, kv_shape, jnp.float32) + value_mean).astype(jnp.bfloat16)
    attn_f32, log_sum_exp = forward_all(queries, key_vecs, value_vecs)
    do_noise = jax.random.normal(key_do, q_shape, jnp.float32)
    grad_out = ((do_noise + 0.5 * attn_f32) * (PREFIX ** 0.5)).astype(jnp.bfloat16)
    return {"queries": queries, "key_vecs": key_vecs, "value_vecs": value_vecs, "attn_out": attn_f32.astype(jnp.bfloat16), "log_sum_exp": log_sum_exp, "grad_out": grad_out}


def reference(queries, key_vecs, value_vecs, attn_out, log_sum_exp, grad_out):
    tile_shape = (BLOCKS, KEY_BLOCK, HEADS_PART, HEAD_DIM)
    key_tiles = key_vecs.astype(jnp.float32).reshape(tile_shape)
    value_tiles = value_vecs.astype(jnp.float32).reshape(tile_shape)
    tile_starts = KEY_BLOCK * jnp.arange(BLOCKS)
    q_shape = (N_QBLOCKS, SEG_BLOCK, HEADS_PART, HEAD_DIM)
    q_blocks = queries.astype(jnp.float32).reshape(q_shape)
    do_blocks = grad_out.astype(jnp.float32).reshape(q_shape)
    row_delta = jnp.sum(grad_out.astype(jnp.float32) * attn_out.astype(jnp.float32), axis=-1)
    delta_blocks = row_delta.reshape(N_QBLOCKS, SEG_BLOCK, HEADS_PART)
    lse_blocks = log_sum_exp.reshape(N_QBLOCKS, SEG_BLOCK, HEADS_PART)
    q_starts = PREFIX0 + SEG_BLOCK * jnp.arange(N_QBLOCKS)

    def query_step(acc_pair, block_in):
        acc_k, acc_v = acc_pair
        q_blk, do_blk, lse_blk, delta_blk, q_start = block_in
        q_pos = q_start + jnp.arange(SEG_BLOCK)
        lse_rows = lse_blk.T[:, :, None]
        delta_rows = delta_blk.T[:, :, None]

        def key_step(dq_acc, tile_in):
            k_tile, v_tile, k_start = tile_in
            k_pos = k_start + jnp.arange(KEY_BLOCK)
            causal = (q_pos[:, None] >= k_pos[None, :])[None]
            scores = jnp.einsum("qhd,khd->hqk", q_blk, k_tile) * SCORE_SCALE
            weights = jnp.where(causal, jnp.exp(scores - lse_rows), 0.0)
            w_bf = weights.astype(jnp.bfloat16).astype(jnp.float32)
            tile_v = jnp.einsum("hqk,qhd->khd", w_bf, do_blk)
            grad_p = jnp.einsum("qhd,khd->hqk", do_blk, v_tile)
            grad_s = (weights * (grad_p - delta_rows)).astype(jnp.bfloat16).astype(jnp.float32)
            dq_acc = dq_acc + jnp.einsum("hqk,khd->qhd", grad_s, k_tile)
            tile_k = jnp.einsum("hqk,qhd->khd", grad_s, q_blk) * SCORE_SCALE
            return dq_acc, (tile_k, tile_v)

        dq_init = jnp.zeros((SEG_BLOCK, HEADS_PART, HEAD_DIM), jnp.float32)
        dq_acc, tile_grads = lax.scan(key_step, dq_init, (key_tiles, value_tiles, tile_starts))
        acc_k = acc_k + tile_grads[0].reshape(PREFIX, HEADS_PART, HEAD_DIM)
        acc_v = acc_v + tile_grads[1].reshape(PREFIX, HEADS_PART, HEAD_DIM)
        return (acc_k, acc_v), (dq_acc * SCORE_SCALE).astype(jnp.bfloat16)

    zero_kv = jnp.zeros((PREFIX, HEADS_PART, HEAD_DIM), jnp.float32)
    kv_grads, dq_blocks = lax.scan(query_step, (zero_kv, zero_kv), (q_blocks, do_blocks, lse_blocks, delta_blocks, q_starts))
    return dq_blocks.reshape(SEGMENTS, SEG_LEN, HEADS_PART, HEAD_DIM), kv_grads[0], kv_grads[1]
```

```python
import functools

import jax
import jax.numpy as jnp
from jax import lax
from jax.experimental import pallas as pl
from jax.experimental.pallas import tpu as pltpu
from jax.sharding import PartitionSpec as P

MESH = pl.DeviceIdType.MESH
CHUNK = 8
LOG2E = 1.4426950408889634


def grid_of(n_chips):
    return {64: (4, 4, 4), 8: (2, 2, 2)}[n_chips]


def rank_of(chip):
    block, place = lax.div(chip, 8), lax.rem(chip, 8)
    z, half = lax.div(block, 2), lax.rem(block, 2)
    idle = lax.rem(z, 2) * 4 + lax.rem(z + half, 4)
    return lax.rem(place + 15 - idle, 8)


def head_of(chip):
    return lax.div(chip, 8) * 7 + rank_of(chip)


def shifted(chip, r, dims, sign):
    nz, ny, nx = dims
    z, y, x = lax.div(chip, ny * nx), lax.rem(lax.div(chip, nx), ny), lax.rem(chip, nx)
    rz, ry, rx = lax.div(r, ny * nx), lax.rem(lax.div(r, nx), ny), lax.rem(r, nx)
    z = lax.rem(z + sign * rz + nz, nz)
    y = lax.rem(y + sign * ry + ny, ny)
    x = lax.rem(x + sign * rx + nx, nx)
    return (z * ny + y) * nx + x


def kernel(n_chips, prefix0, scale, qd_ref, aux_ref, kv_ref, dq_out, dkv_out, qd_buf, aux_buf, kv_buf, row_buf, kpos_buf,
           stage, dqt_acc, dqt_part, dq_stage, qd_send, qd_recv, aux_send, aux_recv, kv_send, kv_recv, pair_send, pair_recv,
           dkv_send, dkv_recv, dq_send, dq_recv, own):
    dims = grid_of(n_chips)
    me = lax.axis_index("cp")
    chip, core = lax.div(me, 2), lax.rem(me, 2)
    partner = (0, chip * 2 + 1 - core)
    q_local = qd_buf.shape[3]
    key_local = kv_buf.shape[2]
    n_chunks = n_chips // CHUNK
    q_blocks = n_chips // 16 if n_chips >= 16 else 1
    q_chips = n_chips // q_blocks
    block = q_chips * q_local
    rows = CHUNK * key_local

    def send_q(r, carry):
        dst = shifted(chip, r, dims, 1)

        @pl.when(rank_of(dst) < 7)
        def _():
            h = head_of(dst)
            there = (0, dst * 2 + core)
            pltpu.make_async_remote_copy(qd_ref.at[h], qd_buf.at[0, chip], qd_send, qd_recv, device_id=there, device_id_type=MESH).start()
            pltpu.make_async_remote_copy(aux_ref.at[h], aux_buf.at[0, chip], aux_send, aux_recv, device_id=there, device_id_type=MESH).start()

        return carry

    def send_kv(r, carry):
        dst = shifted(chip, r, dims, 1)

        @pl.when(rank_of(dst) < 7)
        def _():
            there = (0, dst * 2 + core)
            pltpu.make_async_remote_copy(kv_ref.at[head_of(dst)], kv_buf.at[r], kv_send, kv_recv.at[lax.div(r, CHUNK)],
                                         device_id=there, device_id_type=MESH).start()

        return carry

    lax.fori_loop(1, n_chips, send_q, 0)
    lax.fori_loop(1, n_chips, send_kv, 0)
    active = rank_of(chip) < 7

    def wait_bytes(ref, sem):
        pltpu.make_async_copy(ref, ref, sem).wait()

    @pl.when(active)
    def _():
        my_head = head_of(chip)
        qd_buf[0, chip] = qd_ref[my_head]
        aux_buf[0, chip] = aux_ref[my_head]
        kv_buf[0] = kv_ref[my_head]
        wait_bytes(qd_buf.at[0, pl.ds(0, n_chips - 1)], qd_recv)
        wait_bytes(aux_buf.at[0, pl.ds(0, n_chips - 1)], aux_recv)
        qd_pair = pltpu.make_async_remote_copy(qd_buf.at[0], qd_buf.at[1], pair_send.at[0], pair_recv.at[0], device_id=partner, device_id_type=MESH)
        aux_pair = pltpu.make_async_remote_copy(aux_buf.at[0], aux_buf.at[1], pair_send.at[1], pair_recv.at[1], device_id=partner, device_id_type=MESH)
        qd_pair.start()
        aux_pair.start()

        def make_rows(half):
            for g in range(n_chips // 8):
                row_buf[half, g] = jnp.sum(aux_buf[half, pl.ds(g * 8, 8)], axis=0)

        make_rows(0)
        dqt_acc[...] = jnp.zeros_like(dqt_acc)

        def step(i, carry):
            j, half = lax.div(i, 2), lax.rem(i, 2)

            @pl.when(half == 0)
            def _():
                @pl.when(j == 0)
                def _():
                    wait_bytes(kv_buf.at[pl.ds(1, CHUNK - 1)], kv_recv.at[0])

                @pl.when(j > 0)
                def _():
                    wait_bytes(kv_buf.at[pl.ds(j * CHUNK, CHUNK)], kv_recv.at[j])

                stage[pl.ds(j * CHUNK, CHUNK)] = jnp.zeros((CHUNK,) + stage.shape[1:], jnp.float32)
                for k in range(CHUNK):
                    source = shifted(chip, j * CHUNK + k, dims, -1)
                    first = (source * 2 + core) * key_local - prefix0
                    kpos_buf[pl.ds(k * key_local, key_local)] = first + lax.broadcasted_iota(jnp.int32, (key_local, 128), 0)

            @pl.when(i == 1)
            def _():
                qd_pair.wait()
                aux_pair.wait()
                make_rows(1)

            q_core = lax.rem(core + half, 2)
            keys = kv_buf[pl.ds(j * CHUNK, CHUNK), 0].reshape(rows, 128)
            values = kv_buf[pl.ds(j * CHUNK, CHUNK), 1].reshape(rows, 128)
            keys_t = keys.T

            def q_step(b, carry):
                q = qd_buf[half, pl.ds(b * q_chips, q_chips), 0].reshape(block, 128)
                do = qd_buf[half, pl.ds(b * q_chips, q_chips), 1].reshape(block, 128)
                aux = [row_buf[half, b * (q_chips // 8) + g] for g in range(q_chips // 8)]
                lse2 = jnp.concatenate([a[0:1] for a in aux], axis=1) * LOG2E
                delta = jnp.concatenate([a[1:2] for a in aux], axis=1)
                lane = lax.broadcasted_iota(jnp.int32, (1, block), 1)
                qpos = ((b * q_chips + lax.div(lane, q_local)) * 2 + q_core) * q_local + lax.rem(lane, q_local)
                kpos = jnp.concatenate([kpos_buf[...]] * (block // 128), axis=1)
                s = lax.dot_general(keys, q, (((1,), (1,)), ((), ())), preferred_element_type=jnp.float32)
                p = jnp.where(kpos <= qpos, jnp.exp2(s * (scale * LOG2E) - lse2), 0.0)
                dp = lax.dot_general(values, do, (((1,), (1,)), ((), ())), preferred_element_type=jnp.float32)
                ds = (p * (dp - delta)).astype(jnp.bfloat16)
                dv = jnp.dot(p.astype(jnp.bfloat16), do, preferred_element_type=jnp.float32)
                dk = jnp.dot(ds, q, preferred_element_type=jnp.float32)
                stage[pl.ds(j * CHUNK, CHUNK), 0] += dk.reshape(CHUNK, key_local, 128)
                stage[pl.ds(j * CHUNK, CHUNK), 1] += dv.reshape(CHUNK, key_local, 128)
                dqt_acc[half, b] += jnp.dot(keys_t, ds, preferred_element_type=jnp.float32)
                return carry

            lax.fori_loop(0, q_blocks, q_step, 0)

            @pl.when(half == 1)
            def _():
                stage[pl.ds(j * CHUNK, CHUNK), 0] = stage[pl.ds(j * CHUNK, CHUNK), 0] * scale

                @pl.when(j == 0)
                def _():
                    pltpu.make_async_copy(stage.at[0], dkv_out.at[my_head], own.at[0]).start()

                def send_back(r, carry):
                    source = shifted(chip, r, dims, -1)
                    pltpu.make_async_remote_copy(stage.at[r], dkv_out.at[my_head], dkv_send, dkv_recv,
                                                 device_id=(0, source * 2 + core), device_id_type=MESH).start()
                    return carry

                lax.fori_loop(jnp.maximum(j * CHUNK, 1), j * CHUNK + CHUNK, send_back, 0)

            return carry

        lax.fori_loop(0, 2 * n_chunks, step, 0)

        dq_pair = pltpu.make_async_remote_copy(dqt_acc.at[1], dqt_part, pair_send.at[2], pair_recv.at[2], device_id=partner, device_id_type=MESH)
        dq_pair.start()
        dq_pair.wait()
        for b in range(q_blocks):
            dq = ((dqt_acc[0, b] + dqt_part[b]) * scale).T
            dq_stage[pl.ds(b * q_chips, q_chips)] = dq.astype(jnp.bfloat16).reshape(q_chips, q_local, 128)

        def send_dq(r, carry):
            source = shifted(chip, r, dims, -1)
            pltpu.make_async_remote_copy(dq_stage.at[source], dq_out.at[my_head], dq_send, dq_recv,
                                         device_id=(0, source * 2 + core), device_id_type=MESH).start()
            return carry

        own_dq = pltpu.make_async_copy(dq_stage.at[chip], dq_out.at[my_head], own.at[1])
        own_dq.start()
        lax.fori_loop(1, n_chips, send_dq, 0)
        wait_bytes(stage.at[pl.ds(1, n_chips - 1)], dkv_send)
        wait_bytes(dq_stage.at[pl.ds(1, n_chips - 1)], dq_send)
        pltpu.make_async_copy(stage.at[0], dkv_out.at[my_head], own.at[0]).wait()
        own_dq.wait()

    def finish(count):
        first = pl.ds(0, count)
        wait_bytes(qd_ref.at[first], qd_send)
        wait_bytes(aux_ref.at[first], aux_send)
        wait_bytes(kv_ref.at[first], kv_send)
        wait_bytes(dkv_out.at[first], dkv_recv)
        wait_bytes(dq_out.at[first], dq_recv)

    n_heads = qd_ref.shape[0]

    @pl.when(active)
    def _():
        finish(n_heads - 1)

    @pl.when(jnp.logical_not(active))
    def _():
        finish(n_heads)


def solution(mesh):
    cp_size = mesh.shape["cp"]
    n_chips = cp_size // 2
    spec_q = P(None, "cp", "heads", None)
    spec_kv = P("cp", "heads", None)
    spec_lse = P(None, "cp", "heads")

    def per_device(queries, key_vecs, value_vecs, attn_out, log_sum_exp, grad_out):
        _, q_local, n_heads, head_dim = queries.shape
        key_local = key_vecs.shape[0]
        prefix0 = (key_local - q_local) * cp_size
        scale = head_dim ** -0.5
        place = lax.rem(lax.div(lax.axis_index("cp"), 2), 8)
        row_delta = jnp.einsum("qhd,qhd->qh", grad_out[0], attn_out[0], preferred_element_type=jnp.float32)
        aux = jnp.stack([log_sum_exp[0].T, row_delta.T], axis=1)
        lanes = jnp.arange(128) // q_local
        aux = jnp.where(lanes == place, jnp.tile(aux, (1, 1, 128 // q_local)), 0.0)
        qd = jnp.stack([queries[0], grad_out[0]]).transpose(2, 0, 1, 3)
        kv = jnp.stack([key_vecs, value_vecs]).transpose(2, 0, 1, 3)
        q_blocks = n_chips // 16 if n_chips >= 16 else 1
        block = n_chips // q_blocks * q_local
        n_chunks = n_chips // CHUNK
        bf16, f32 = jnp.bfloat16, jnp.float32
        dma = pltpu.SemaphoreType.DMA
        dq, dkv = pl.pallas_call(
            functools.partial(kernel, n_chips, prefix0, scale),
            name="exchange_and_backward",
            out_shape=(jax.ShapeDtypeStruct((n_heads, q_local, head_dim), bf16), jax.ShapeDtypeStruct((n_heads, 2, key_local, head_dim), f32)),
            in_specs=[pl.BlockSpec(memory_space=pltpu.VMEM)] * 3,
            out_specs=[pl.BlockSpec(memory_space=pl.ANY)] * 2,
            scratch_shapes=[
                pltpu.VMEM((2, n_chips, 2, q_local, head_dim), bf16),
                pltpu.VMEM((2, n_chips, 2, 128), f32),
                pltpu.VMEM((n_chips, 2, key_local, head_dim), bf16),
                pltpu.VMEM((2, n_chips // 8, 2, 128), f32),
                pltpu.VMEM((CHUNK * key_local, 128), jnp.int32),
                pltpu.VMEM((n_chips, 2, key_local, head_dim), f32),
                pltpu.VMEM((2, q_blocks, head_dim, block), f32),
                pltpu.VMEM((q_blocks, head_dim, block), f32),
                pltpu.VMEM((n_chips, q_local, head_dim), bf16),
                dma, dma, dma, dma, dma, dma((n_chunks,)), dma((3,)), dma((3,)), dma, dma, dma, dma, dma((2,)),
            ],
            compiler_params=pltpu.CompilerParams(has_side_effects=True, vmem_limit_bytes=56 * 1024 * 1024),
        )(qd, aux, kv)
        grad_q = dq.transpose(1, 0, 2)[None]
        return grad_q, dkv[:, 0].transpose(1, 0, 2), dkv[:, 1].transpose(1, 0, 2)

    return jax.shard_map(per_device, mesh=mesh, in_specs=(spec_q, spec_kv, spec_kv, spec_q, spec_lse, spec_q), out_specs=(spec_q, spec_kv, spec_kv), check_vma=False)
```

```python
import functools

import jax
import jax.numpy as jnp
from jax import lax
from jax.experimental import pallas as pl
from jax.experimental.pallas import tpu as pltpu
from jax.sharding import PartitionSpec as P

MESH = pl.DeviceIdType.MESH
GROUPS = 4
LINE_AXIS = (0, 1, 2, 0)
FIRST_AXIS = (1, 2, 0, 2)
SECOND_AXIS = (2, 0, 1, 1)
LOG2E = 1.4426950408889634
FORWARD_LAG = 2
STORE_LAG = 4
F32, BF16 = jnp.float32, jnp.bfloat16


def pick(table, g):
    if isinstance(g, int):
        return table[g]
    value = table[-1]
    for k in range(len(table) - 1):
        value = jnp.where(g == k, table[k], value)
    return value


def rank_at(n, a, b):
    size = 8 if n == 4 else 4
    pos = a * n + b
    block, place = lax.div(pos, size), lax.rem(pos, size)
    rank = lax.rem(place + 2 * size - 1 - block * 2, size)
    return block * (size - 1) + rank, rank < size - 1


class Spot:
    def __init__(self, n, coords, chip, core, g):
        strides = (n * n, n, 1)
        self.n, self.chip, self.core = n, chip, core
        self.s_line, self.s_a, self.s_b = (pick([strides[t[k]] for k in range(GROUPS)], g) for t in (LINE_AXIS, FIRST_AXIS, SECOND_AXIS))
        self.line, self.a, self.b = (pick([coords[t[k]] for k in range(GROUPS)], g) for t in (LINE_AXIS, FIRST_AXIS, SECOND_AXIS))

    def turn(self, c, d):
        return lax.rem(c + d + self.n, self.n)

    def at(self, a=0, b=0, line=0):
        return (self.chip + (self.turn(self.a, a) - self.a) * self.s_a + (self.turn(self.b, b) - self.b) * self.s_b
                + (self.turn(self.line, line) - self.line) * self.s_line)

    def device(self, a=0, b=0, line=0):
        return (0, self.at(a, b, line) * 2 + self.core)

    def rank(self, a=0, b=0):
        return rank_at(self.n, self.turn(self.a, a), self.turn(self.b, b))


def kernel(n, prefix0, scale, n_heads, q_in, k_in, v_in, o_in, lse_in, do_in, dq_out, dk_out, dv_out,
           q_raw, k_raw, v_raw, o_raw, lse_raw, do_raw, q_f32, do_f32, k_f32, v_f32, lse_pad, aux_rows,
           q_src, aux_src, kv_src, qd, aux, rows, kv1, kv2, kpos_buf, res, ret1, ret2, dqt, part, line_sum, dq_src, dq_got,
           dq_f32, dk_f32, dv_f32, dq_bf,
           in_sem, q_send, q_recv, aux_send, aux_recv, ql_send, ql_recv, al_send, al_recv, pair_send, pair_recv, k1_send, k1_recv,
           k2_send, k2_recv, r1_send, r1_recv, r2_send, r2_recv, part_send, part_recv, ls_send, ls_recv, dq_send, dq_recv, out_sem):
    me = lax.axis_index("cp")
    chip, core = lax.div(me, 2), lax.rem(me, 2)
    coords = (lax.div(chip, n * n), lax.rem(lax.div(chip, n), n), lax.rem(chip, n))
    partner = (0, chip * 2 + 1 - core)
    spots = [Spot(n, coords, chip, core, g) for g in range(GROUPS)]
    holds = [s.rank()[1] for s in spots]
    heads = n_heads // GROUPS
    q_local, key_local = q_src.shape[3], kv_src.shape[4]
    plane = n * n
    unit_rows = min(8, plane)
    width = unit_rows * q_local
    block = plane * q_local
    n_rows = block // width
    keys_in = n * key_local

    def remote(src, dst, send, recv, device):
        return pltpu.make_async_remote_copy(src, dst, send, recv, device_id=device, device_id_type=MESH)

    def wait_bytes(ref, sem):
        pltpu.make_async_copy(ref, ref, sem).wait()

    loads = [pltpu.make_async_copy(a, b, in_sem.at[k]) for k, (a, b) in enumerate(
        [(q_in, q_raw), (do_in, do_raw), (o_in, o_raw), (lse_in, lse_raw), (k_in, k_raw), (v_in, v_raw)])]
    for copy in loads:
        copy.start()

    barrier = pltpu.get_barrier_semaphore()
    met = 1
    pl.semaphore_signal(barrier, inc=1, device_id=partner, device_id_type=MESH)
    for g, spot in enumerate(spots[:3]):
        for a in range(n):
            for b in range(1, n):
                pl.semaphore_signal(barrier, inc=1, device_id=spot.device(a, b), device_id_type=MESH)
                met += 1

    def widen(src, dst, count):
        per = n_heads * 4

        def go(t, carry):
            at = pl.ds(pl.multiple_of(t * per, 8), per)
            dst[at] = src[at].astype(F32)
            return carry

        lax.fori_loop(0, count // 4, go, 0)

    for copy in loads[:4]:
        copy.wait()
    widen(q_raw, q_f32, q_local)
    widen(do_raw, do_f32, q_local)
    lse_pad[0:q_local, 0:n_heads] = lse_raw[...]
    lse_t = lse_pad[...].T[0:n_heads]
    head_group = lax.div(lax.broadcasted_iota(jnp.int32, (n_heads, 128), 0), heads)
    lane = lax.broadcasted_iota(jnp.int32, (n_heads, 128), 1)
    base = pick([lax.rem(s.b * n + s.a, unit_rows) * q_local for s in spots], head_group)
    row_lse, row_delta = jnp.zeros((n_heads, 128), F32), jnp.zeros((n_heads, 128), F32)
    for t in range(q_local):
        at = pl.ds(t * n_heads, n_heads)
        delta = jnp.sum(do_f32[at] * o_raw[at].astype(F32), axis=1, keepdims=True)
        row_delta = jnp.where(lane == base + t, delta, row_delta)
        row_lse = jnp.where(lane == base + t, lse_t[:, t:t + 1], row_lse)
    aux_rows[0] = row_lse
    aux_rows[1] = row_delta

    def lay_out_q(i, carry):
        g = lax.div(i, plane)
        spot = Spot(n, coords, chip, core, g)
        rank, _ = spot.rank(lax.div(lax.rem(i, plane), n), lax.rem(i, n))
        h = g * heads + lax.rem(rank, heads)
        u = lax.rem(i, plane)
        q_src[g, u, 0] = q_f32[pl.ds(h, q_local, stride=n_heads), :].astype(BF16)
        q_src[g, u, 1] = do_f32[pl.ds(h, q_local, stride=n_heads), :].astype(BF16)
        aux_src[g, u, 0:1] = aux_rows[0, pl.ds(h, 1), :]
        aux_src[g, u, 1:2] = aux_rows[1, pl.ds(h, 1), :]
        return carry

    lax.fori_loop(0, GROUPS * plane, lay_out_q, 0)
    for copy in loads[4:]:
        copy.wait()
    widen(k_raw, k_f32, key_local)
    widen(v_raw, v_f32, key_local)

    def lay_out_kv(i, carry):
        g = lax.div(i, plane)
        spot = Spot(n, coords, chip, core, g)
        d1, d2 = lax.div(lax.rem(i, plane), n), lax.rem(i, n)
        rank, _ = spot.rank(d1, d2)
        h = g * heads + lax.rem(rank, heads)
        kv_src[g, d1, d2, 0] = k_f32[pl.ds(h, key_local, stride=n_heads), :].astype(BF16)
        kv_src[g, d1, d2, 1] = v_f32[pl.ds(h, key_local, stride=n_heads), :].astype(BF16)
        return carry

    lax.fori_loop(0, GROUPS * plane, lay_out_kv, 0)
    pl.semaphore_wait(barrier, met)

    def send_q():
        def go(i, carry):
            g, u = lax.div(i, plane), lax.rem(i, plane)
            spot = Spot(n, coords, chip, core, g)
            d1, d2 = lax.div(u, n), lax.rem(u, n)

            @pl.when(jnp.logical_and(u > 0, spot.rank(d1, d2)[1]))
            def _():
                there = spot.device(d1, d2)
                remote(q_src.at[g, u], qd.at[g, 0, spot.line, spot.b, spot.a], q_send.at[g], q_recv.at[g], there).start()
                remote(aux_src.at[g, u], aux.at[g, 0, spot.line, spot.b, spot.a], aux_send.at[g], aux_recv.at[g], there).start()

            return carry

        lax.fori_loop(0, GROUPS * plane, go, 0)

    def k_first(g):
        for d in range(1, n):
            remote(kv_src.at[g, d], kv1.at[g, d], k1_send.at[g], k1_recv.at[g], spots[g].device(a=d)).start()

    def k_second(g, own):
        for d in range(1, n):
            @pl.when(spots[g].rank(b=d)[1])
            def _():
                there = spots[g].device(b=d)
                if own:
                    remote(kv_src.at[g, 0, d], kv2.at[g, d, 0], k2_send.at[g, d], k2_recv.at[g, d], there).start()
                else:
                    remote(kv1.at[g, pl.ds(1, n - 1), d], kv2.at[g, d, pl.ds(1, n - 1)], k2_send.at[g, d], k2_recv.at[g, d], there).start()

    def q_line(g):
        for d in range(1, n):
            there = spots[g].device(line=d)
            remote(qd.at[g, 0, spots[g].line], qd.at[g, 0, spots[g].line], ql_send.at[g], ql_recv.at[g], there).start()
            remote(aux.at[g, 0, spots[g].line], aux.at[g, 0, spots[g].line], al_send.at[g], al_recv.at[g], there).start()

    send_q()
    for g in range(GROUPS):
        k_first(g)
    for g in range(GROUPS):
        k_second(g, True)
    for g, spot in enumerate(spots):
        @pl.when(holds[g])
        def _():
            qd[g, 0, spot.line, spot.b, spot.a] = q_src[g, 0]
            aux[g, 0, spot.line, spot.b, spot.a] = aux_src[g, 0]
            wait_bytes(q_src.at[g, pl.ds(1, plane - 1)], q_recv.at[g])
            wait_bytes(aux_src.at[g, pl.ds(1, plane - 1)], aux_recv.at[g])
            q_line(g)

    for g in range(GROUPS):
        wait_bytes(kv1.at[g, pl.ds(1, n - 1)], k1_recv.at[g])
        k_second(g, False)

    def pair_copies(g):
        return (remote(qd.at[g, 0], qd.at[g, 1], pair_send.at[0, g], pair_recv.at[0, g], partner),
                remote(aux.at[g, 0], aux.at[g, 1], pair_send.at[1, g], pair_recv.at[1, g], partner))

    def share_queries(g):
        wait_bytes(qd.at[g, 0, pl.ds(0, n - 1)], ql_recv.at[g])
        wait_bytes(aux.at[g, 0, pl.ds(0, n - 1)], al_recv.at[g])
        for copy in pair_copies(g):
            copy.start()

    @pl.when(holds[0])
    def _():
        share_queries(0)

    n_chunks = GROUPS * n

    def chunk_of(i):
        g = lax.div(i, n)
        return g, lax.rem(lax.rem(i, n) + jnp.where(g == GROUPS - 1, 1, 0), n)

    def compute(i):
        g, o2 = chunk_of(i)
        spot = Spot(n, coords, chip, core, g)

        @pl.when(lax.rem(i, n) == 0)
        def _():
            for copy in pair_copies(g):
                copy.wait()
            for half in range(2):
                for l in range(n):
                    units = aux[g, half, l].reshape(n_rows, unit_rows, 2, 128)
                    rows[half, l] = jnp.sum(units, axis=1)
            dqt[g] = jnp.zeros(dqt.shape[1:], F32)

        @pl.when(o2 == 0)
        def _():
            kv2[g, 0, 0] = kv_src[g, 0, 0]
            for o1 in range(1, n):
                kv2[g, 0, o1] = kv1[g, o1, 0]

        @pl.when(o2 > 0)
        def _():
            wait_bytes(kv2.at[g, o2], k2_recv.at[g, o2])

        for o1 in range(n):
            first = (spot.at(a=-o1, b=-o2) * 2 + core) * key_local - prefix0
            kpos_buf[pl.ds(o1 * key_local, key_local)] = first + lax.broadcasted_iota(jnp.int32, (key_local, 128), 0)
        keys = kv2[g, o2, :, 0].reshape(keys_in, 128)
        values = kv2[g, o2, :, 1].reshape(keys_in, 128)
        keys_t = keys.T
        res[g, o2] = jnp.zeros(res.shape[2:], F32)

        def q_step(s, carry):
            half = lax.rem(s, 2)
            l = spot.turn(spot.line, 1 + lax.div(s, 2))
            q = qd[g, half, l, :, :, 0].reshape(block, 128)
            do = qd[g, half, l, :, :, 1].reshape(block, 128)
            lse2 = jnp.concatenate([rows[half, l, r, 0:1, 0:width] for r in range(n_rows)], axis=1) * LOG2E
            delta = jnp.concatenate([rows[half, l, r, 1:2, 0:width] for r in range(n_rows)], axis=1)
            lanes = lax.broadcasted_iota(jnp.int32, (1, block), 1)
            unit = lax.div(lanes, q_local)
            q_chip = l * spot.s_line + lax.div(unit, n) * spot.s_b + lax.rem(unit, n) * spot.s_a
            qpos = (q_chip * 2 + lax.rem(core + half, 2)) * q_local + lax.rem(lanes, q_local)
            kpos = jnp.concatenate([kpos_buf[...]] * n_rows, axis=1)[:, 0:block]
            s_ = lax.dot_general(keys, q, (((1,), (1,)), ((), ())), preferred_element_type=F32)
            p = jnp.where(kpos <= qpos, jnp.exp2(s_ * (scale * LOG2E) - lse2), 0.0)
            dp = lax.dot_general(values, do, (((1,), (1,)), ((), ())), preferred_element_type=F32)
            ds = (p * (dp - delta)).astype(BF16)
            res[g, o2, :, 0] += jnp.dot(ds, q, preferred_element_type=F32).reshape(n, key_local, 128)
            res[g, o2, :, 1] += jnp.dot(p.astype(BF16), do, preferred_element_type=F32).reshape(n, key_local, 128)
            dqt[g, half, l] += jnp.dot(keys_t, ds, preferred_element_type=F32)
            return carry

        lax.fori_loop(0, 2 * n, q_step, 0)
        res[g, o2, :, 0] = res[g, o2, :, 0] * scale

    def part_copy(g):
        return remote(dqt.at[g, 1], part.at[g], part_send.at[g], part_recv.at[g], partner)

    def line_copy(g, spot, d):
        return remote(dqt.at[g, 0, spot.turn(spot.line, d)], line_sum.at[g, n - 1 - d], ls_send.at[g], ls_recv.at[g], spot.device(line=d))

    def dq_copy(g, spot, u):
        b, a = spot.turn(spot.b, lax.div(u, n)), spot.turn(spot.a, lax.rem(u, n))
        h = g * heads + lax.rem(spot.rank()[0], heads)
        return remote(dq_src.at[g, b * n + a], dq_got.at[h], dq_send.at[g], dq_recv.at[g], spot.device(a=lax.rem(u, n), b=lax.div(u, n)))

    def first_back(g, o2, spot):
        return remote(res.at[g, o2], ret1.at[g, o2], r1_send.at[g, o2], r1_recv.at[g, o2], spot.device(b=-o2))

    def second_back(g, o2, o1, spot, src):
        return remote(src.at[g, o2, o1], ret2.at[g, o2, o1], r2_send.at[g, o2], r2_recv.at[g, o2, o1], spot.device(a=-o1))

    def step(i, carry):
        @pl.when(i < n_chunks)
        def _():
            g, o2 = chunk_of(i)
            spot = Spot(n, coords, chip, core, g)

            @pl.when(spot.rank()[1])
            def _():
                compute(i)

                @pl.when(o2 > 0)
                def _():
                    first_back(g, o2, spot).start()

                @pl.when(o2 == 0)
                def _():
                    for o1 in range(1, n):
                        second_back(g, 0, o1, spot, res).start()

        @pl.when(jnp.logical_and(lax.rem(i, n) == n - 1, i < n_chunks))
        def _():
            g = lax.div(i, n)

            @pl.when(Spot(n, coords, chip, core, g).rank()[1])
            def _():
                part_copy(g).start()

        @pl.when(jnp.logical_and(lax.rem(i, n) == 0, jnp.logical_and(i >= n, i <= n_chunks)))
        def _():
            g = lax.div(i, n) - 1
            spot = Spot(n, coords, chip, core, g)

            @pl.when(spot.rank()[1])
            def _():
                part_copy(g).wait()
                for l in range(n):
                    dqt[g, 0, l] = dqt[g, 0, l] + part[g, l]
                for d in range(1, n):
                    line_copy(g, spot, d).start()

        @pl.when(jnp.logical_and(lax.rem(i, n) == 1, jnp.logical_and(i >= n, i <= n_chunks + 1)))
        def _():
            g = lax.div(i, n) - 1
            spot = Spot(n, coords, chip, core, g)

            @pl.when(spot.rank()[1])
            def _():
                wait_bytes(line_sum.at[g], ls_recv.at[g])
                total = dqt[g, 0, spot.line]
                for d in range(n - 1):
                    total = total + line_sum[g, d]
                dq_src[g] = (total * scale).T.astype(BF16).reshape(plane, q_local, 128)
                h = g * heads + spot.rank()[0]
                dq_got[h] = dq_src[g, spot.b * n + spot.a]

                def go(u, carry):
                    dq_copy(g, spot, u).start()
                    return carry

                lax.fori_loop(1, plane, go, 0)

        @pl.when(jnp.logical_and(lax.rem(i, n) == n - 2, i < n_chunks - n))
        def _():
            g = lax.div(i, n) + 1

            @pl.when(Spot(n, coords, chip, core, g).rank()[1])
            def _():
                share_queries(g)

        j = i - FORWARD_LAG

        @pl.when(jnp.logical_and(j >= 0, j < n_chunks))
        def _():
            g, o2 = chunk_of(j)
            spot = Spot(n, coords, chip, core, g)

            @pl.when(jnp.logical_and(o2 > 0, spot.rank(b=o2)[1]))
            def _():
                wait_bytes(ret1.at[g, o2], r1_recv.at[g, o2])
                for o1 in range(1, n):
                    second_back(g, o2, o1, spot, ret1).start()

        k = i - STORE_LAG

        @pl.when(k >= 0)
        def _():
            g, o2 = chunk_of(k)
            spot = Spot(n, coords, chip, core, g)

            def put(o1, src):
                rank, _ = spot.rank(a=o1, b=o2)
                at = pl.ds(g * heads + rank, key_local, stride=n_heads)
                dk_f32[at, :] = src[g, o2, o1, 0]
                dv_f32[at, :] = src[g, o2, o1, 1]

            for o1 in range(n):
                @pl.when(spot.rank(a=o1, b=o2)[1])
                def _():
                    if o1:
                        wait_bytes(ret2.at[g, o2, o1], r2_recv.at[g, o2, o1])
                        return
                    pl.when(o2 == 0)(lambda: put(0, res))
                    pl.when(o2 > 0)(lambda: put(0, ret1))

            for o1 in range(1, n):
                @pl.when(spot.rank(a=o1, b=o2)[1])
                def _():
                    put(o1, ret2)

        return carry

    lax.fori_loop(0, n_chunks + STORE_LAG, step, 0)

    outs = [pltpu.make_async_copy(dk_f32, dk_out, out_sem.at[0]), pltpu.make_async_copy(dv_f32, dv_out, out_sem.at[1])]
    for copy in outs:
        copy.start()
    for g in range(GROUPS):
        for mine in (False, True):
            @pl.when(holds[g] if mine else jnp.logical_not(holds[g]))
            def _():
                wait_bytes(dq_got.at[pl.ds(0, heads - mine)], dq_recv.at[g])

    def put_dq(h, carry):
        dq_f32[pl.ds(h, q_local, stride=n_heads), :] = dq_got[h].astype(F32)
        return carry

    lax.fori_loop(0, n_heads, put_dq, 0)
    dq_bf[...] = dq_f32[...].astype(BF16)
    dq_copy_out = pltpu.make_async_copy(dq_bf, dq_out, out_sem.at[2])
    dq_copy_out.start()

    for g, spot in enumerate(spots):
        for mine in (False, True):
            @pl.when(holds[g] if mine else jnp.logical_not(holds[g]))
            def _():
                wait_bytes(q_src.at[g, pl.ds(0, heads - mine)], q_send.at[g])
                wait_bytes(aux_src.at[g, pl.ds(0, heads - mine)], aux_send.at[g])
        wait_bytes(kv1.at[g, pl.ds(1, n - 1)], k1_send.at[g])

        @pl.when(holds[g])
        def _():
            wait_bytes(qd.at[g, 0, pl.ds(0, n - 1)], ql_send.at[g])
            wait_bytes(aux.at[g, 0, pl.ds(0, n - 1)], al_send.at[g])
            wait_bytes(line_sum.at[g], ls_send.at[g])
            wait_bytes(dq_src.at[g, pl.ds(1, plane - 1)], dq_send.at[g])
            wait_bytes(res.at[g, 0, pl.ds(1, n - 1)], r2_send.at[g, 0])
            for d in range(1, n):
                wait_bytes(res.at[g, d], r1_send.at[g, d])

        for d in range(1, n):
            @pl.when(spot.rank(b=d)[1])
            def _():
                wait_bytes(kv2.at[g, d], k2_send.at[g, d])
                wait_bytes(res.at[g, d, pl.ds(1, n - 1)], r2_send.at[g, d])

    for copy in outs:
        copy.wait()
    dq_copy_out.wait()


def solution(mesh):
    cp_size = mesh.shape["cp"]
    n = {128: 4, 16: 2}[cp_size]
    spec_q = P(None, "cp", "heads", None)
    spec_kv = P("cp", "heads", None)
    spec_lse = P(None, "cp", "heads")

    def per_device(queries, key_vecs, value_vecs, attn_out, log_sum_exp, grad_out):
        _, q_local, n_heads, dim = queries.shape
        key_local = key_vecs.shape[0]
        prefix0 = (key_local - q_local) * cp_size
        plane, block = n * n, n * n * q_local
        q_rows, k_rows = q_local * n_heads, key_local * n_heads
        unit_rows = min(8, plane)
        dma = pltpu.SemaphoreType.DMA
        g4 = GROUPS
        vmem = pltpu.VMEM
        scratch = [
            vmem((q_rows, dim), BF16), vmem((k_rows, dim), BF16), vmem((k_rows, dim), BF16), vmem((q_rows, dim), BF16),
            vmem((q_local, n_heads), F32), vmem((q_rows, dim), BF16),
            vmem((q_rows, dim), F32), vmem((q_rows, dim), F32), vmem((k_rows, dim), F32), vmem((k_rows, dim), F32),
            vmem((128, 128), F32), vmem((2, n_heads, 128), F32),
            vmem((g4, plane, 2, q_local, dim), BF16), vmem((g4, plane, 2, 128), F32), vmem((g4, n, n, 2, key_local, dim), BF16),
            vmem((g4, 2, n, n, n, 2, q_local, dim), BF16), vmem((g4, 2, n, n, n, 2, 128), F32),
            vmem((2, n, plane // unit_rows, 2, 128), F32),
            vmem((g4, n, n, 2, key_local, dim), BF16), vmem((g4, n, n, 2, key_local, dim), BF16), vmem((n * key_local, 128), jnp.int32),
            vmem((g4, n, n, 2, key_local, dim), F32), vmem((g4, n, n, 2, key_local, dim), F32), vmem((g4, n, n, 2, key_local, dim), F32),
            vmem((g4, 2, n, dim, block), F32), vmem((g4, n, dim, block), F32), vmem((g4, n - 1, dim, block), F32),
            vmem((g4, plane, q_local, dim), BF16), vmem((n_heads, q_local, dim), BF16),
            vmem((q_rows, dim), F32), vmem((k_rows, dim), F32), vmem((k_rows, dim), F32), vmem((q_rows, dim), BF16),
            dma((6,)), dma((g4,)), dma((g4,)), dma((g4,)), dma((g4,)), dma((g4,)), dma((g4,)), dma((g4,)), dma((g4,)), dma((2, g4)), dma((2, g4)),
            dma((g4,)), dma((g4,)),
            dma((g4, n)), dma((g4, n)), dma((g4, n)), dma((g4, n)), dma((g4, n)), dma((g4, n, n)), dma((g4,)), dma((g4,)), dma((g4,)), dma((g4,)), dma((g4,)), dma((g4,)),
            dma((3,)),
        ]
        anywhere = pl.BlockSpec(memory_space=pl.ANY)
        dq, dk, dv = pl.pallas_call(
            functools.partial(kernel, n, prefix0, dim ** -0.5, n_heads),
            name="exchange_and_backward",
            out_shape=(jax.ShapeDtypeStruct((q_rows, dim), BF16), jax.ShapeDtypeStruct((k_rows, dim), F32), jax.ShapeDtypeStruct((k_rows, dim), F32)),
            in_specs=[anywhere] * 6,
            out_specs=[anywhere] * 3,
            scratch_shapes=scratch,
            compiler_params=pltpu.CompilerParams(has_side_effects=True, collective_id=0, vmem_limit_bytes=60 * 1024 * 1024),
        )(queries.reshape(q_rows, dim), key_vecs.reshape(k_rows, dim), value_vecs.reshape(k_rows, dim), attn_out.reshape(q_rows, dim),
          log_sum_exp[0], grad_out.reshape(q_rows, dim))
        return dq.reshape(queries.shape), dk.reshape(key_vecs.shape), dv.reshape(value_vecs.shape)

    return jax.shard_map(per_device, mesh=mesh, in_specs=(spec_q, spec_kv, spec_kv, spec_q, spec_lse, spec_q), out_specs=(spec_q, spec_kv, spec_kv), check_vma=False)
```

```python
import functools

import jax
import jax.numpy as jnp
from jax import lax
from jax.experimental import pallas as pl
from jax.experimental.pallas import tpu as pltpu
from jax.sharding import PartitionSpec as P

MESH = pl.DeviceIdType.MESH
GROUPS = 4
LINE_AXIS = (0, 1, 2, 0)
FIRST_AXIS = (1, 2, 0, 2)
SECOND_AXIS = (2, 0, 1, 1)
LOG2E = 1.4426950408889634
FORWARD_LAG = 2
STORE_LAG = 4
F32, BF16 = jnp.float32, jnp.bfloat16


def pick(table, g):
    if isinstance(g, int):
        return table[g]
    return (sum(v << (4 * k) for k, v in enumerate(table)) >> (4 * g)) & 15


def rank_at(n, a, b):
    if n == 2:
        rank = (a * 2 + b + 3) & 3
        return rank, rank < 3
    block = a >> 1
    rank = (((a & 1) << 2) + b + 7 - 2 * block) & 7
    return block * 7 + rank, rank < 7


class Spot:
    def __init__(self, n, chip, core, g):
        bits = n // 2
        self.n, self.chip, self.core = n, chip, core
        self.s_line, self.s_a, self.s_b = (pick([(2 - axis) * bits for axis in table], g) for table in (LINE_AXIS, FIRST_AXIS, SECOND_AXIS))
        self.line, self.a, self.b = ((chip >> s) & (n - 1) for s in (self.s_line, self.s_a, self.s_b))

    def turn(self, c, d):
        return (c + d) & (self.n - 1)

    def at(self, a=0, b=0, line=0):
        chip = self.chip
        for c, d, s in ((self.a, a, self.s_a), (self.b, b, self.s_b), (self.line, line, self.s_line)):
            if not (isinstance(d, int) and d == 0):
                chip = chip + ((self.turn(c, d) - c) << s)
        return chip

    def device(self, a=0, b=0, line=0):
        return (0, self.at(a, b, line) * 2 + self.core)

    def rank(self, a=0, b=0):
        return rank_at(self.n, self.turn(self.a, a), self.turn(self.b, b))


def kernel(n, prefix0, scale, n_heads, q_in, k_in, v_in, o_in, lse_in, do_in, dq_out, dk_out, dv_out,
           q_raw, k_raw, v_raw, o_raw, lse_raw, do_raw, q_f32, do_f32, k_f32, v_f32, lse_pad, aux_rows,
           q_src, aux_src, kv_src, qd, aux, rows, kv1, kv2, kpos_buf, res, ret1, ret2, dqt, part, line_sum, dq_src, dq_got,
           dq_f32, dk_f32, dv_f32, dq_bf, p_buf, ds_buf,
           in_sem, q_send, q_recv, aux_send, aux_recv, ql_send, ql_recv, al_send, al_recv, pair_send, pair_recv, k1_send, k1_recv,
           k2_send, k2_recv, r1_send, r1_recv, r2_send, r2_recv, part_send, part_recv, ls_send, ls_recv, dq_send, dq_recv, out_sem):
    me = lax.axis_index("cp")
    chip, core = me >> 1, me & 1
    bits = n // 2
    partner = (0, chip * 2 + 1 - core)
    spots = [Spot(n, chip, core, g) for g in range(GROUPS)]
    holds = [s.rank()[1] for s in spots]
    heads = n_heads // GROUPS
    q_local, key_local = q_src.shape[3], kv_src.shape[4]
    plane = n * n
    unit_rows = min(8, plane)
    width = unit_rows * q_local
    block = plane * q_local
    n_rows = block // width
    keys_in = n * key_local

    def remote(src, dst, send, recv, device):
        return pltpu.make_async_remote_copy(src, dst, send, recv, device_id=device, device_id_type=MESH)

    def wait_bytes(ref, sem):
        pltpu.make_async_copy(ref, ref, sem).wait()

    loads = [pltpu.make_async_copy(a, b, in_sem.at[k]) for k, (a, b) in enumerate(
        [(q_in, q_raw), (do_in, do_raw), (o_in, o_raw), (lse_in, lse_raw), (k_in, k_raw), (v_in, v_raw)])]
    for copy in loads:
        copy.start()

    barrier = pltpu.get_barrier_semaphore()
    met = 1
    pl.semaphore_signal(barrier, inc=1, device_id=partner, device_id_type=MESH)
    for g, spot in enumerate(spots[:3]):
        for a in range(n):
            for b in range(1, n):
                pl.semaphore_signal(barrier, inc=1, device_id=spot.device(a, b), device_id_type=MESH)
                met += 1

    def widen(src, dst, count):
        per = n_heads * 4

        def go(t, carry):
            at = pl.ds(pl.multiple_of(t * per, 8), per)
            dst[at] = src[at].astype(F32)
            return carry

        lax.fori_loop(0, count // 4, go, 0)

    for copy in loads[:4]:
        copy.wait()
    widen(q_raw, q_f32, q_local)
    widen(do_raw, do_f32, q_local)
    lse_pad[0:q_local, 0:n_heads] = lse_raw[...]
    lse_t = lse_pad[...].T[0:n_heads]
    head_group = lax.div(lax.broadcasted_iota(jnp.int32, (n_heads, 128), 0), heads)
    lane = lax.broadcasted_iota(jnp.int32, (n_heads, 128), 1)
    base = jnp.zeros((n_heads, 128), jnp.int32)
    for g, spot in enumerate(spots):
        base = jnp.where(head_group == g, ((spot.b * n + spot.a) & (unit_rows - 1)) * q_local, base)
    row_lse, row_delta = jnp.zeros((n_heads, 128), F32), jnp.zeros((n_heads, 128), F32)
    for t in range(q_local):
        at = pl.ds(t * n_heads, n_heads)
        delta = jnp.sum(do_f32[at] * o_raw[at].astype(F32), axis=1, keepdims=True)
        row_delta = jnp.where(lane == base + t, delta, row_delta)
        row_lse = jnp.where(lane == base + t, lse_t[:, t:t + 1], row_lse)
    aux_rows[0] = row_lse
    aux_rows[1] = row_delta

    for g, spot in enumerate(spots):
        def lay_out_q(u, carry):
            rank, _ = spot.rank(u >> bits, u & (n - 1))
            h = g * heads + jnp.minimum(rank, heads - 1)
            q_src[g, u, 0] = q_f32[pl.ds(h, q_local, stride=n_heads), :].astype(BF16)
            q_src[g, u, 1] = do_f32[pl.ds(h, q_local, stride=n_heads), :].astype(BF16)
            aux_src[g, u, 0:1] = aux_rows[0, pl.ds(h, 1), :]
            aux_src[g, u, 1:2] = aux_rows[1, pl.ds(h, 1), :]
            return carry

        lax.fori_loop(0, plane, lay_out_q, 0, unroll=8)
    for copy in loads[4:]:
        copy.wait()
    widen(k_raw, k_f32, key_local)
    widen(v_raw, v_f32, key_local)

    for g, spot in enumerate(spots):
        def lay_out_kv(u, carry):
            rank, _ = spot.rank(u >> bits, u & (n - 1))
            h = g * heads + jnp.minimum(rank, heads - 1)
            kv_src[g, u >> bits, u & (n - 1), 0] = k_f32[pl.ds(h, key_local, stride=n_heads), :].astype(BF16)
            kv_src[g, u >> bits, u & (n - 1), 1] = v_f32[pl.ds(h, key_local, stride=n_heads), :].astype(BF16)
            return carry

        lax.fori_loop(0, plane, lay_out_kv, 0, unroll=4)
    pl.semaphore_wait(barrier, met)

    def send_q(g):
        spot = spots[g]
        for u in range(1, plane):
            d1, d2 = u >> bits, u & (n - 1)

            @pl.when(spot.rank(d1, d2)[1])
            def _():
                there = spot.device(d1, d2)
                remote(q_src.at[g, u], qd.at[g, 0, spot.line, spot.b, spot.a], q_send.at[g], q_recv.at[g], there).start()
                remote(aux_src.at[g, u], aux.at[g, 0, spot.line, spot.b, spot.a], aux_send.at[g], aux_recv.at[g], there).start()

    def k_first(g):
        for d in range(1, n):
            remote(kv_src.at[g, d], kv1.at[g, d], k1_send.at[g], k1_recv.at[g], spots[g].device(a=d)).start()

    def k_second(g, own):
        for d in range(1, n):
            @pl.when(spots[g].rank(b=d)[1])
            def _():
                there = spots[g].device(b=d)
                if own:
                    remote(kv_src.at[g, 0, d], kv2.at[g, d, 0], k2_send.at[g, d], k2_recv.at[g, d], there).start()
                else:
                    remote(kv1.at[g, pl.ds(1, n - 1), d], kv2.at[g, d, pl.ds(1, n - 1)], k2_send.at[g, d], k2_recv.at[g, d], there).start()

    def q_line(g):
        for d in range(1, n):
            there = spots[g].device(line=d)
            remote(qd.at[g, 0, spots[g].line], qd.at[g, 0, spots[g].line], ql_send.at[g], ql_recv.at[g], there).start()
            remote(aux.at[g, 0, spots[g].line], aux.at[g, 0, spots[g].line], al_send.at[g], al_recv.at[g], there).start()

    def meet_plane(g):
        spot = spots[g]

        @pl.when(holds[g])
        def _():
            qd[g, 0, spot.line, spot.b, spot.a] = q_src[g, 0]
            aux[g, 0, spot.line, spot.b, spot.a] = aux_src[g, 0]
            wait_bytes(q_src.at[g, pl.ds(1, plane - 1)], q_recv.at[g])
            wait_bytes(aux_src.at[g, pl.ds(1, plane - 1)], aux_recv.at[g])
            q_line(g)

    for g in range(GROUPS):
        send_q(g)
        if g < 2:
            k_first(g)
            k_second(g, True)
    meet_plane(0)
    for g in range(2, GROUPS):
        k_first(g)
        k_second(g, True)
    for g in range(1, GROUPS):
        meet_plane(g)
    for g in range(GROUPS):
        wait_bytes(kv1.at[g, pl.ds(1, n - 1)], k1_recv.at[g])
        k_second(g, False)

    def pair_copies(g):
        return (remote(qd.at[g, 0], qd.at[g, 1], pair_send.at[0, g], pair_recv.at[0, g], partner),
                remote(aux.at[g, 0], aux.at[g, 1], pair_send.at[1, g], pair_recv.at[1, g], partner))

    def share_queries(g):
        wait_bytes(qd.at[g, 0, pl.ds(0, n - 1)], ql_recv.at[g])
        wait_bytes(aux.at[g, 0, pl.ds(0, n - 1)], al_recv.at[g])
        for copy in pair_copies(g):
            copy.start()

    @pl.when(holds[0])
    def _():
        share_queries(0)

    n_chunks = GROUPS * n

    def chunk_of(i):
        g = i >> bits
        return g, (i + jnp.where(g == GROUPS - 1, 1, 0)) & (n - 1)

    def compute(i):
        g, o2 = chunk_of(i)
        spot = Spot(n, chip, core, g)

        @pl.when((i & (n - 1)) == 0)
        def _():
            for copy in pair_copies(g):
                copy.wait()
            for half in range(2):
                for l in range(n):
                    units = aux[g, half, l].reshape(n_rows, unit_rows, 2, 128)
                    rows[half, l] = jnp.sum(units, axis=1)
            dqt[g] = jnp.zeros(dqt.shape[1:], F32)

        @pl.when(o2 == 0)
        def _():
            kv2[g, 0, 0] = kv_src[g, 0, 0]
            for o1 in range(1, n):
                kv2[g, 0, o1] = kv1[g, o1, 0]

        @pl.when(o2 > 0)
        def _():
            wait_bytes(kv2.at[g, o2], k2_recv.at[g, o2])

        for o1 in range(n):
            first = (spot.at(a=-o1, b=-o2) * 2 + core) * key_local - prefix0
            kpos_buf[pl.ds(o1 * key_local, key_local)] = first + lax.broadcasted_iota(jnp.int32, (key_local, 128), 0)
        keys = kv2[g, o2, :, 0].reshape(keys_in, 128)
        values = kv2[g, o2, :, 1].reshape(keys_in, 128)
        keys_t = keys.T

        def q_step(s, carry):
            half = s & 1
            l = spot.turn(spot.line, 1 + (s >> 1))
            q = qd[g, half, l, :, :, 0].reshape(block, 128)
            do = qd[g, half, l, :, :, 1].reshape(block, 128)
            lse2 = jnp.concatenate([rows[half, l, r, 0:1, 0:width] for r in range(n_rows)], axis=1) * LOG2E
            delta = jnp.concatenate([rows[half, l, r, 1:2, 0:width] for r in range(n_rows)], axis=1)
            lanes = lax.broadcasted_iota(jnp.int32, (1, block), 1)
            unit = lax.div(lanes, q_local)
            q_chip = (l << spot.s_line) + (lax.div(unit, n) << spot.s_b) + (lax.rem(unit, n) << spot.s_a)
            qpos = (q_chip * 2 + ((core + half) & 1)) * q_local + lax.rem(lanes, q_local)
            kpos = jnp.concatenate([kpos_buf[...]] * n_rows, axis=1)[:, 0:block]
            s_ = lax.dot_general(keys, q, (((1,), (1,)), ((), ())), preferred_element_type=F32)
            p = jnp.where(kpos <= qpos, jnp.exp2(s_ * (scale * LOG2E) - lse2), 0.0)
            dp = lax.dot_general(values, do, (((1,), (1,)), ((), ())), preferred_element_type=F32)
            ds = (p * (dp - delta)).astype(BF16)
            at = pl.ds(pl.multiple_of((half * n + l) * block, block), block)
            p_buf[:, at] = p.astype(BF16)
            ds_buf[:, at] = ds
            return carry

        lax.fori_loop(0, 2 * n, q_step, 0, unroll=8)
        q_all = qd[g, :, :, :, :, 0].reshape(2 * n * block, 128)
        do_all = qd[g, :, :, :, :, 1].reshape(2 * n * block, 128)
        for half in range(2):
            for l in range(n):
                at = pl.ds((half * n + l) * block, block)
                dqt[g, half, l] += jnp.dot(keys_t, ds_buf[:, at], preferred_element_type=F32)
        res[g, o2, :, 0] = (jnp.dot(ds_buf[...], q_all, preferred_element_type=F32) * scale).reshape(n, key_local, 128)
        res[g, o2, :, 1] = jnp.dot(p_buf[...], do_all, preferred_element_type=F32).reshape(n, key_local, 128)

    def part_copy(g):
        return remote(dqt.at[g, 1], part.at[g], part_send.at[g], part_recv.at[g], partner)

    def line_copy(g, spot, d):
        return remote(dqt.at[g, 0, spot.turn(spot.line, d)], line_sum.at[g, n - 1 - d], ls_send.at[g], ls_recv.at[g], spot.device(line=d))

    def dq_copy(g, spot, u):
        b, a = spot.turn(spot.b, u >> bits), spot.turn(spot.a, u & (n - 1))
        h = g * heads + jnp.minimum(spot.rank()[0], heads - 1)
        return remote(dq_src.at[g, b * n + a], dq_got.at[h], dq_send.at[g], dq_recv.at[g], spot.device(a=u & (n - 1), b=u >> bits))

    def first_back(g, o2, spot):
        return remote(res.at[g, o2], ret1.at[g, o2], r1_send.at[g, o2], r1_recv.at[g, o2], spot.device(b=-o2))

    def second_back(g, o2, o1, spot, src):
        return remote(src.at[g, o2, o1], ret2.at[g, o2, o1], r2_send.at[g, o2], r2_recv.at[g, o2, o1], spot.device(a=-o1))

    def step(i, carry):
        @pl.when(i < n_chunks)
        def _():
            g, o2 = chunk_of(i)
            spot = Spot(n, chip, core, g)

            @pl.when(spot.rank()[1])
            def _():
                compute(i)

                @pl.when(o2 > 0)
                def _():
                    first_back(g, o2, spot).start()

                @pl.when(o2 == 0)
                def _():
                    for o1 in range(1, n):
                        second_back(g, 0, o1, spot, res).start()

        @pl.when(jnp.logical_and((i & (n - 1)) == n - 1, i < n_chunks))
        def _():
            g = (i >> bits)

            @pl.when(Spot(n, chip, core, g).rank()[1])
            def _():
                part_copy(g).start()

        @pl.when(jnp.logical_and((i & (n - 1)) == 0, jnp.logical_and(i >= n, i <= n_chunks)))
        def _():
            g = (i >> bits) - 1
            spot = Spot(n, chip, core, g)

            @pl.when(spot.rank()[1])
            def _():
                part_copy(g).wait()
                for l in range(n):
                    dqt[g, 0, l] = dqt[g, 0, l] + part[g, l]
                for d in range(1, n):
                    line_copy(g, spot, d).start()

        @pl.when(jnp.logical_and((i & (n - 1)) == 1, jnp.logical_and(i >= n, i <= n_chunks + 1)))
        def _():
            g = (i >> bits) - 1
            spot = Spot(n, chip, core, g)

            @pl.when(spot.rank()[1])
            def _():
                wait_bytes(line_sum.at[g], ls_recv.at[g])
                total = dqt[g, 0, spot.line]
                for d in range(n - 1):
                    total = total + line_sum[g, d]
                dq_src[g] = (total * scale).T.astype(BF16).reshape(plane, q_local, 128)
                h = g * heads + spot.rank()[0]
                dq_got[h] = dq_src[g, spot.b * n + spot.a]

                def go(u, carry):
                    dq_copy(g, spot, u).start()
                    return carry

                lax.fori_loop(1, plane, go, 0)

        @pl.when(jnp.logical_and((i & (n - 1)) == n - 2, i < n_chunks - n))
        def _():
            g = (i >> bits) + 1

            @pl.when(Spot(n, chip, core, g).rank()[1])
            def _():
                share_queries(g)

        j = i - FORWARD_LAG

        @pl.when(jnp.logical_and(j >= 0, j < n_chunks))
        def _():
            g, o2 = chunk_of(j)
            spot = Spot(n, chip, core, g)

            @pl.when(jnp.logical_and(o2 > 0, spot.rank(b=o2)[1]))
            def _():
                wait_bytes(ret1.at[g, o2], r1_recv.at[g, o2])
                for o1 in range(1, n):
                    second_back(g, o2, o1, spot, ret1).start()

        k = i - STORE_LAG

        @pl.when(k >= 0)
        def _():
            g, o2 = chunk_of(k)
            spot = Spot(n, chip, core, g)

            def put(o1, src):
                rank, _ = spot.rank(a=o1, b=o2)
                at = pl.ds(g * heads + rank, key_local, stride=n_heads)
                dk_f32[at, :] = src[g, o2, o1, 0]
                dv_f32[at, :] = src[g, o2, o1, 1]

            for o1 in range(n):
                @pl.when(spot.rank(a=o1, b=o2)[1])
                def _():
                    if o1:
                        wait_bytes(ret2.at[g, o2, o1], r2_recv.at[g, o2, o1])
                        return
                    pl.when(o2 == 0)(lambda: put(0, res))
                    pl.when(o2 > 0)(lambda: put(0, ret1))

            for o1 in range(1, n):
                @pl.when(spot.rank(a=o1, b=o2)[1])
                def _():
                    put(o1, ret2)

        return carry

    lax.fori_loop(0, n_chunks + STORE_LAG, step, 0)

    outs = [pltpu.make_async_copy(dk_f32, dk_out, out_sem.at[0]), pltpu.make_async_copy(dv_f32, dv_out, out_sem.at[1])]
    for copy in outs:
        copy.start()
    for g in range(GROUPS):
        for mine in (False, True):
            @pl.when(holds[g] if mine else jnp.logical_not(holds[g]))
            def _():
                wait_bytes(dq_got.at[pl.ds(0, heads - mine)], dq_recv.at[g])

    def put_dq(h, carry):
        dq_f32[pl.ds(h, q_local, stride=n_heads), :] = dq_got[h].astype(F32)
        return carry

    lax.fori_loop(0, n_heads, put_dq, 0)
    dq_bf[...] = dq_f32[...].astype(BF16)
    dq_copy_out = pltpu.make_async_copy(dq_bf, dq_out, out_sem.at[2])
    dq_copy_out.start()

    for g, spot in enumerate(spots):
        for mine in (False, True):
            @pl.when(holds[g] if mine else jnp.logical_not(holds[g]))
            def _():
                wait_bytes(q_src.at[g, pl.ds(0, heads - mine)], q_send.at[g])
                wait_bytes(aux_src.at[g, pl.ds(0, heads - mine)], aux_send.at[g])
        wait_bytes(kv1.at[g, pl.ds(1, n - 1)], k1_send.at[g])

        @pl.when(holds[g])
        def _():
            wait_bytes(qd.at[g, 0, pl.ds(0, n - 1)], ql_send.at[g])
            wait_bytes(aux.at[g, 0, pl.ds(0, n - 1)], al_send.at[g])
            wait_bytes(line_sum.at[g], ls_send.at[g])
            wait_bytes(dq_src.at[g, pl.ds(1, plane - 1)], dq_send.at[g])
            wait_bytes(res.at[g, 0, pl.ds(1, n - 1)], r2_send.at[g, 0])
            for d in range(1, n):
                wait_bytes(res.at[g, d], r1_send.at[g, d])

        for d in range(1, n):
            @pl.when(spot.rank(b=d)[1])
            def _():
                wait_bytes(kv2.at[g, d], k2_send.at[g, d])
                wait_bytes(res.at[g, d, pl.ds(1, n - 1)], r2_send.at[g, d])

    for copy in outs:
        copy.wait()
    dq_copy_out.wait()


def solution(mesh):
    cp_size = mesh.shape["cp"]
    n = {128: 4, 16: 2}[cp_size]
    spec_q = P(None, "cp", "heads", None)
    spec_kv = P("cp", "heads", None)
    spec_lse = P(None, "cp", "heads")

    def per_device(queries, key_vecs, value_vecs, attn_out, log_sum_exp, grad_out):
        _, q_local, n_heads, dim = queries.shape
        key_local = key_vecs.shape[0]
        prefix0 = (key_local - q_local) * cp_size
        plane, block = n * n, n * n * q_local
        q_rows, k_rows = q_local * n_heads, key_local * n_heads
        unit_rows = min(8, plane)
        dma = pltpu.SemaphoreType.DMA
        g4 = GROUPS
        vmem = pltpu.VMEM
        scratch = [
            vmem((q_rows, dim), BF16), vmem((k_rows, dim), BF16), vmem((k_rows, dim), BF16), vmem((q_rows, dim), BF16),
            vmem((q_local, n_heads), F32), vmem((q_rows, dim), BF16),
            vmem((q_rows, dim), F32), vmem((q_rows, dim), F32), vmem((k_rows, dim), F32), vmem((k_rows, dim), F32),
            vmem((128, 128), F32), vmem((2, n_heads, 128), F32),
            vmem((g4, plane, 2, q_local, dim), BF16), vmem((g4, plane, 2, 128), F32), vmem((g4, n, n, 2, key_local, dim), BF16),
            vmem((g4, 2, n, n, n, 2, q_local, dim), BF16), vmem((g4, 2, n, n, n, 2, 128), F32),
            vmem((2, n, plane // unit_rows, 2, 128), F32),
            vmem((g4, n, n, 2, key_local, dim), BF16), vmem((g4, n, n, 2, key_local, dim), BF16), vmem((n * key_local, 128), jnp.int32),
            vmem((g4, n, n, 2, key_local, dim), F32), vmem((g4, n, n, 2, key_local, dim), F32), vmem((g4, n, n, 2, key_local, dim), F32),
            vmem((g4, 2, n, dim, block), F32), vmem((g4, n, dim, block), F32), vmem((g4, n - 1, dim, block), F32),
            vmem((g4, plane, q_local, dim), BF16), vmem((n_heads, q_local, dim), BF16),
            vmem((q_rows, dim), F32), vmem((k_rows, dim), F32), vmem((k_rows, dim), F32), vmem((q_rows, dim), BF16),
            vmem((n * key_local, 2 * n * block), BF16), vmem((n * key_local, 2 * n * block), BF16),
            dma((6,)), dma((g4,)), dma((g4,)), dma((g4,)), dma((g4,)), dma((g4,)), dma((g4,)), dma((g4,)), dma((g4,)), dma((2, g4)), dma((2, g4)),
            dma((g4,)), dma((g4,)),
            dma((g4, n)), dma((g4, n)), dma((g4, n)), dma((g4, n)), dma((g4, n)), dma((g4, n, n)), dma((g4,)), dma((g4,)), dma((g4,)), dma((g4,)), dma((g4,)), dma((g4,)),
            dma((3,)),
        ]
        anywhere = pl.BlockSpec(memory_space=pl.ANY)
        dq, dk, dv = pl.pallas_call(
            functools.partial(kernel, n, prefix0, dim ** -0.5, n_heads),
            name="exchange_and_backward",
            out_shape=(jax.ShapeDtypeStruct((q_rows, dim), BF16), jax.ShapeDtypeStruct((k_rows, dim), F32), jax.ShapeDtypeStruct((k_rows, dim), F32)),
            in_specs=[anywhere] * 6,
            out_specs=[anywhere] * 3,
            scratch_shapes=scratch,
            compiler_params=pltpu.CompilerParams(has_side_effects=True, collective_id=0, vmem_limit_bytes=60 * 1024 * 1024),
        )(queries.reshape(q_rows, dim), key_vecs.reshape(k_rows, dim), value_vecs.reshape(k_rows, dim), attn_out.reshape(q_rows, dim),
          log_sum_exp[0], grad_out.reshape(q_rows, dim))
        return dq.reshape(queries.shape), dk.reshape(key_vecs.shape), dv.reshape(value_vecs.shape)

    return jax.shard_map(per_device, mesh=mesh, in_specs=(spec_q, spec_kv, spec_kv, spec_q, spec_lse, spec_q), out_specs=(spec_q, spec_kv, spec_kv), check_vma=False)
```

```python
import functools

import jax
import jax.numpy as jnp
from jax import lax
from jax.experimental import pallas as pl
from jax.experimental.pallas import tpu as pltpu
from jax.sharding import PartitionSpec as P

MESH = pl.DeviceIdType.MESH
GROUPS = 4
LINE_AXIS, FIRST_AXIS, SECOND_AXIS = zip((1, 0, 2), (2, 1, 0), (0, 2, 1), (0, 1, 2))
CHUNKS = ((3, 1), (3, 3), (3, 0), (3, 2), (2, 2), (0, 1), (0, 3), (0, 0), (1, 0), (1, 1), (1, 3), (0, 2), (2, 3), (2, 1), (1, 2), (2, 0))
BEFORE = (("q1", 3), ("q1", 1), ("q1", 2), ("q1", 0), ("k1", 3), ("k1", 0), ("q2", 3), ("q2", 1), ("q2", 0), ("k1", 2), ("k2", 0), ("line", 3),
          ("q2", 2), ("line", 0), ("k2", 3), ("line", 2), ("k1", 1), ("line", 1), ("k2", 2))
AFTER = {2: (("k2", 1),)}
LOG2E = 1.4426950408889634
FORWARD_LAG = 6
SUM_LAG = 7
STORE_LAG = 16
VMEM_MIB = 46
F32, BF16 = jnp.float32, jnp.bfloat16


def pick(table, g):
    if isinstance(g, int):
        return table[g]
    return (sum(v << (4 * k) for k, v in enumerate(table)) >> (4 * g)) & 15


def rank_at(n, a, b):
    if n == 2:
        rank = (a * 2 + b + 3) & 3
        return rank, rank < 3
    block = a >> 1
    rank = (((a & 1) << 2) + b + 7 - 2 * block) & 7
    return block * 7 + rank, rank < 7


class Spot:
    def __init__(self, n, chip, core, g):
        bits = n // 2
        self.n, self.chip, self.core = n, chip, core
        self.s_line, self.s_a, self.s_b = (pick([(2 - axis) * bits for axis in table], g) for table in (LINE_AXIS, FIRST_AXIS, SECOND_AXIS))
        self.line, self.a, self.b = ((chip >> s) & (n - 1) for s in (self.s_line, self.s_a, self.s_b))

    def turn(self, c, d):
        return (c + d) & (self.n - 1)

    def at(self, a=0, b=0, line=0):
        chip = self.chip
        for c, d, s in ((self.a, a, self.s_a), (self.b, b, self.s_b), (self.line, line, self.s_line)):
            if not (isinstance(d, int) and d == 0):
                chip = chip + ((self.turn(c, d) - c) << s)
        return chip

    def device(self, a=0, b=0, line=0):
        return (0, self.at(a, b, line) * 2 + self.core)

    def rank(self, a=0, b=0):
        return rank_at(self.n, self.turn(self.a, a), self.turn(self.b, b))


def kernel(n, prefix0, scale, n_heads, q_raw, k_raw, v_raw, o_raw, lse_raw, do_raw, dq_bf, dk_f32, dv_f32,
           q_f32, do_f32, k_f32, v_f32, lse_pad, aux_rows,
           q_src, aux_src, kv_src, q1, qd, aux, rows, kv1, kv2, kpos_buf, res, ret1, ret2, dqt, part, line_sum, dq_src, dq_got,
           dq_f32, p_buf, ds_buf,
           q1_send, q1_recv, q2_send, q2_recv, aux_send, aux_recv, ql_send, ql_recv, al_send, al_recv, pair_send, pair_recv, k1_send, k1_recv,
           k2_send, k2_recv, r1_send, r1_recv, r2_send, r2_recv, part_send, part_recv, ls_send, ls_recv, dq_send, dq_recv):
    me = lax.axis_index("cp")
    chip, core = me >> 1, me & 1
    bits = n // 2
    partner = (0, chip * 2 + 1 - core)
    spots = [Spot(n, chip, core, g) for g in range(GROUPS)]
    holds = [s.rank()[1] for s in spots]
    heads = n_heads // GROUPS
    q_local, key_local = q_src.shape[4], kv_src.shape[4]
    plane = n * n
    unit_rows = min(8, plane)
    width = unit_rows * q_local
    block = plane * q_local
    n_rows = block // width
    keys_in = n * key_local

    def remote(src, dst, send, recv, device):
        return pltpu.make_async_remote_copy(src, dst, send, recv, device_id=device, device_id_type=MESH)

    def wait_bytes(ref, sem):
        pltpu.make_async_copy(ref, ref, sem).wait()

    barrier = pltpu.get_barrier_semaphore()
    met = 1
    pl.semaphore_signal(barrier, inc=1, device_id=partner, device_id_type=MESH)
    for g, spot in enumerate(spots[:3]):
        for a in range(n):
            for b in range(1, n):
                pl.semaphore_signal(barrier, inc=1, device_id=spot.device(a, b), device_id_type=MESH)
                met += 1

    def widen(src, dst, count):
        per = n_heads * 4

        def go(t, carry):
            at = pl.ds(pl.multiple_of(t * per, 8), per)
            dst[at] = src[at].astype(F32)
            return carry

        lax.fori_loop(0, count // 4, go, 0)

    widen(q_raw, q_f32, q_local)
    widen(do_raw, do_f32, q_local)
    lse_pad[0:q_local, 0:n_heads] = lse_raw[...]
    lse_t = lse_pad[...].T[0:n_heads]
    head_group = lax.div(lax.broadcasted_iota(jnp.int32, (n_heads, 128), 0), heads)
    lane = lax.broadcasted_iota(jnp.int32, (n_heads, 128), 1)
    base = jnp.zeros((n_heads, 128), jnp.int32)
    for g, spot in enumerate(spots):
        base = jnp.where(head_group == g, ((spot.b * n + spot.a) & (unit_rows - 1)) * q_local, base)
    row_lse, row_delta = jnp.zeros((n_heads, 128), F32), jnp.zeros((n_heads, 128), F32)
    for t in range(q_local):
        at = pl.ds(t * n_heads, n_heads)
        delta = jnp.sum(do_f32[at] * o_raw[at].astype(F32), axis=1, keepdims=True)
        row_delta = jnp.where(lane == base + t, delta, row_delta)
        row_lse = jnp.where(lane == base + t, lse_t[:, t:t + 1], row_lse)
    aux_rows[0] = row_lse
    aux_rows[1] = row_delta

    for g, spot in enumerate(spots):
        def lay_out_q(u, carry):
            rank, _ = spot.rank(u >> bits, u & (n - 1))
            h = g * heads + jnp.minimum(rank, heads - 1)
            q_src[g, u >> bits, u & (n - 1), 0] = q_f32[pl.ds(h, q_local, stride=n_heads), :].astype(BF16)
            q_src[g, u >> bits, u & (n - 1), 1] = do_f32[pl.ds(h, q_local, stride=n_heads), :].astype(BF16)
            aux_src[g, u, 0:1] = aux_rows[0, pl.ds(h, 1), :]
            aux_src[g, u, 1:2] = aux_rows[1, pl.ds(h, 1), :]
            return carry

        lax.fori_loop(0, plane, lay_out_q, 0, unroll=8)
    widen(k_raw, k_f32, key_local)
    widen(v_raw, v_f32, key_local)

    for g, spot in enumerate(spots):
        def lay_out_kv(u, carry):
            rank, _ = spot.rank(u >> bits, u & (n - 1))
            h = g * heads + jnp.minimum(rank, heads - 1)
            kv_src[g, u >> bits, u & (n - 1), 0] = k_f32[pl.ds(h, key_local, stride=n_heads), :].astype(BF16)
            kv_src[g, u >> bits, u & (n - 1), 1] = v_f32[pl.ds(h, key_local, stride=n_heads), :].astype(BF16)
            return carry

        lax.fori_loop(0, plane, lay_out_kv, 0, unroll=4)
    pl.semaphore_wait(barrier, met)

    def q_first(g):
        spot = spots[g]
        for d in range(1, n):
            remote(q_src.at[g, d], q1.at[g, d], q1_send.at[g], q1_recv.at[g], spot.device(a=d)).start()
        for u in range(1, plane):
            d1, d2 = u >> bits, u & (n - 1)

            @pl.when(spot.rank(d1, d2)[1])
            def _():
                remote(aux_src.at[g, u], aux.at[g, 0, spot.line, spot.b, spot.a], aux_send.at[g], aux_recv.at[g], spot.device(d1, d2)).start()

    def q_second(g):
        spot = spots[g]
        wait_bytes(q1.at[g, pl.ds(1, n - 1)], q1_recv.at[g])

        @pl.when(holds[g])
        def _():
            for o1 in range(n):
                qd[g, 0, spot.line, spot.b, spot.turn(spot.a, -o1)] = q1[g, o1, 0] if o1 else q_src[g, 0, 0]
            aux[g, 0, spot.line, spot.b, spot.a] = aux_src[g, 0]

        for d in range(1, n):
            @pl.when(spot.rank(b=d)[1])
            def _():
                there = spot.device(b=d)
                for o1 in range(n):
                    src = q1.at[g, o1, d] if o1 else q_src.at[g, 0, d]
                    remote(src, qd.at[g, 0, spot.line, spot.b, spot.turn(spot.a, -o1)], q2_send.at[g, d], q2_recv.at[g], there).start()

    def k_first(g):
        for d in range(1, n):
            remote(kv_src.at[g, d], kv1.at[g, d], k1_send.at[g], k1_recv.at[g], spots[g].device(a=d)).start()

    def k_second(g, own):
        for d in range(1, n):
            @pl.when(spots[g].rank(b=d)[1])
            def _():
                there = spots[g].device(b=d)
                if own:
                    remote(kv_src.at[g, 0, d], kv2.at[g, d, 0], k2_send.at[g, d], k2_recv.at[g, d], there).start()
                else:
                    remote(kv1.at[g, pl.ds(1, n - 1), d], kv2.at[g, d, pl.ds(1, n - 1)], k2_send.at[g, d], k2_recv.at[g, d], there).start()

    def q_line(g):
        for d in range(1, n):
            there = spots[g].device(line=d)
            remote(qd.at[g, 0, spots[g].line], qd.at[g, 0, spots[g].line], ql_send.at[g], ql_recv.at[g], there).start()
            remote(aux.at[g, 0, spots[g].line], aux.at[g, 0, spots[g].line], al_send.at[g], al_recv.at[g], there).start()

    def line_out(g):
        @pl.when(holds[g])
        def _():
            wait_bytes(q_src.at[g, pl.ds(1, n - 1)], q2_recv.at[g])
            wait_bytes(aux_src.at[g, pl.ds(1, plane - 1)], aux_recv.at[g])
            q_line(g)

    def pass_on(g):
        wait_bytes(kv1.at[g, pl.ds(1, n - 1)], k1_recv.at[g])
        k_second(g, False)

    def keys_out(g):
        k_first(g)
        k_second(g, True)

    def pair_copies(g):
        return (remote(qd.at[g, 0], qd.at[g, 1], pair_send.at[0, g], pair_recv.at[0, g], partner),
                remote(aux.at[g, 0], aux.at[g, 1], pair_send.at[1, g], pair_recv.at[1, g], partner))

    def share_queries(g):
        wait_bytes(qd.at[g, 0, pl.ds(0, n - 1)], ql_recv.at[g])
        wait_bytes(aux.at[g, 0, pl.ds(0, n - 1)], al_recv.at[g])
        for copy in pair_copies(g):
            copy.start()

    acts = {"q1": q_first, "q2": q_second, "k1": keys_out, "k2": pass_on, "line": line_out}
    chunks = [(g, o2) for g, o2 in CHUNKS if o2 < n]
    n_chunks = len(chunks)
    first = [min(k for k, c in enumerate(chunks) if c[0] == g) for g in range(GROUPS)]
    last = [max(k for k, c in enumerate(chunks) if c[0] == g) for g in range(GROUPS)]
    after = {k: list(v) for k, v in AFTER.items()} if n == 4 else {-1: [a for v in AFTER.values() for a in v]}
    lined = {g: k for k, v in after.items() for name, g in v if name == "line"}
    for name, g in list(BEFORE) + after.pop(-1, []):
        acts[name](g)
    shares = {g: max(first[g] - 2, lined.get(g, -1), -1) for g in range(GROUPS)}

    def share(g):
        pl.when(holds[g])(lambda: share_queries(g))

    for g in range(GROUPS):
        if shares[g] < 0:
            share(g)
    codes = [sum((g * 4 + o2) << (4 * k) for k, (g, o2) in enumerate(chunks[w:w + 8])) for w in range(0, n_chunks, 8)]
    codes = [c - (1 << 32) if c >= 1 << 31 else c for c in codes]
    begins = sum(1 << k for k in first)

    def chunk_of(i):
        word = codes[0] if len(codes) == 1 else jnp.where(i < 8, codes[0], codes[1])
        code = word >> (4 * (i & 7))
        return (code >> 2) & 3, code & 3

    def compute(i):
        g, o2 = chunk_of(i)
        spot = Spot(n, chip, core, g)

        @pl.when(((begins >> i) & 1) == 1)
        def _():
            for copy in pair_copies(g):
                copy.wait()
            for half in range(2):
                for l in range(n):
                    units = aux[g, half, l].reshape(n_rows, unit_rows, 2, 128)
                    rows[g, half, l] = jnp.sum(units, axis=1)
            dqt[g] = jnp.zeros(dqt.shape[1:], F32)

        @pl.when(o2 == 0)
        def _():
            kv2[g, 0, 0] = kv_src[g, 0, 0]
            for o1 in range(1, n):
                kv2[g, 0, o1] = kv1[g, o1, 0]

        @pl.when(o2 > 0)
        def _():
            wait_bytes(kv2.at[g, o2], k2_recv.at[g, o2])

        for o1 in range(n):
            first = (spot.at(a=-o1, b=-o2) * 2 + core) * key_local - prefix0
            kpos_buf[pl.ds(o1 * key_local, key_local)] = first + lax.broadcasted_iota(jnp.int32, (key_local, 128), 0)
        keys = kv2[g, o2, :, 0].reshape(keys_in, 128)
        values = kv2[g, o2, :, 1].reshape(keys_in, 128)
        keys_t = keys.T

        def q_step(s, carry):
            half = s & 1
            l = spot.turn(spot.line, 1 + (s >> 1))
            q = qd[g, half, l, :, :, 0].reshape(block, 128)
            do = qd[g, half, l, :, :, 1].reshape(block, 128)
            lse2 = jnp.concatenate([rows[g, half, l, r, 0:1, 0:width] for r in range(n_rows)], axis=1) * LOG2E
            delta = jnp.concatenate([rows[g, half, l, r, 1:2, 0:width] for r in range(n_rows)], axis=1)
            lanes = lax.broadcasted_iota(jnp.int32, (1, block), 1)
            unit = lax.div(lanes, q_local)
            q_chip = (l << spot.s_line) + (lax.div(unit, n) << spot.s_b) + (lax.rem(unit, n) << spot.s_a)
            qpos = (q_chip * 2 + ((core + half) & 1)) * q_local + lax.rem(lanes, q_local)
            kpos = jnp.concatenate([kpos_buf[...]] * n_rows, axis=1)[:, 0:block]
            s_ = lax.dot_general(keys, q, (((1,), (1,)), ((), ())), preferred_element_type=F32)
            p = jnp.where(kpos <= qpos, jnp.exp2(s_ * (scale * LOG2E) - lse2), 0.0)
            dp = lax.dot_general(values, do, (((1,), (1,)), ((), ())), preferred_element_type=F32)
            ds = (p * (dp - delta)).astype(BF16)
            at = pl.ds(pl.multiple_of((half * n + l) * block, block), block)
            p_buf[:, at] = p.astype(BF16)
            ds_buf[:, at] = ds
            return carry

        lax.fori_loop(0, 2 * n, q_step, 0, unroll=8)
        q_all = qd[g, :, :, :, :, 0].reshape(2 * n * block, 128)
        do_all = qd[g, :, :, :, :, 1].reshape(2 * n * block, 128)
        for half in range(2):
            for l in range(n):
                at = pl.ds((half * n + l) * block, block)
                dqt[g, half, l] += jnp.dot(keys_t, ds_buf[:, at], preferred_element_type=F32)
        res[g, o2, :, 0] = (jnp.dot(ds_buf[...], q_all, preferred_element_type=F32) * scale).reshape(n, key_local, 128)
        res[g, o2, :, 1] = jnp.dot(p_buf[...], do_all, preferred_element_type=F32).reshape(n, key_local, 128)

    def part_copy(g):
        return remote(dqt.at[g, 1], part.at[g], part_send.at[g], part_recv.at[g], partner)

    def line_copy(g, spot, d):
        return remote(dqt.at[g, 0, spot.turn(spot.line, d)], line_sum.at[g, n - 1 - d], ls_send.at[g], ls_recv.at[g], spot.device(line=d))

    def dq_copy(g, spot, u):
        b, a = spot.turn(spot.b, u >> bits), spot.turn(spot.a, u & (n - 1))
        h = g * heads + jnp.minimum(spot.rank()[0], heads - 1)
        return remote(dq_src.at[g, b * n + a], dq_got.at[h], dq_send.at[g], dq_recv.at[g], spot.device(a=u & (n - 1), b=u >> bits))

    def first_back(g, o2, spot):
        return remote(res.at[g, o2], ret1.at[g, o2], r1_send.at[g, o2], r1_recv.at[g, o2], spot.device(b=-o2))

    def second_back(g, o2, o1, spot, src):
        return remote(src.at[g, o2, o1], ret2.at[g, o2, o1], r2_send.at[g, o2], r2_recv.at[g, o2, o1], spot.device(a=-o1))

    def step(i, carry):
        @pl.when(i < n_chunks)
        def _():
            g, o2 = chunk_of(i)
            spot = Spot(n, chip, core, g)

            @pl.when(spot.rank()[1])
            def _():
                compute(i)

                @pl.when(o2 > 0)
                def _():
                    first_back(g, o2, spot).start()

                @pl.when(o2 == 0)
                def _():
                    for o1 in range(1, n):
                        second_back(g, 0, o1, spot, res).start()

        for k, todo in after.items():
            @pl.when(i == k)
            def _():
                for name, g in todo:
                    acts[name](g)

        for g, spot in enumerate(spots):
            @pl.when(jnp.logical_and(i == last[g], holds[g]))
            def _():
                part_copy(g).start()

            @pl.when(jnp.logical_and(i == last[g] + 1, holds[g]))
            def _():
                part_copy(g).wait()
                for l in range(n):
                    dqt[g, 0, l] = dqt[g, 0, l] + part[g, l]
                for d in range(1, n):
                    line_copy(g, spot, d).start()

            @pl.when(jnp.logical_and(i == last[g] + 1 + SUM_LAG, holds[g]))
            def _():
                wait_bytes(line_sum.at[g], ls_recv.at[g])
                total = dqt[g, 0, spot.line]
                for d in range(n - 1):
                    total = total + line_sum[g, d]
                dq_src[g] = (total * scale).T.astype(BF16).reshape(plane, q_local, 128)
                h = g * heads + spot.rank()[0]
                dq_got[h] = dq_src[g, spot.b * n + spot.a]

                def go(u, carry):
                    dq_copy(g, spot, u).start()
                    return carry

                lax.fori_loop(1, plane, go, 0)

            if shares[g] >= 0:
                @pl.when(i == shares[g])
                def _():
                    share(g)

        j = i - FORWARD_LAG

        @pl.when(jnp.logical_and(j >= 0, j < n_chunks))
        def _():
            g, o2 = chunk_of(j)
            spot = Spot(n, chip, core, g)

            @pl.when(jnp.logical_and(o2 > 0, spot.rank(b=o2)[1]))
            def _():
                wait_bytes(ret1.at[g, o2], r1_recv.at[g, o2])
                for o1 in range(1, n):
                    second_back(g, o2, o1, spot, ret1).start()

        k = i - STORE_LAG

        @pl.when(jnp.logical_and(k >= 0, k < n_chunks))
        def _():
            g, o2 = chunk_of(k)
            spot = Spot(n, chip, core, g)

            def put(o1, src):
                rank, _ = spot.rank(a=o1, b=o2)
                at = pl.ds(g * heads + rank, key_local, stride=n_heads)
                dk_f32[at, :] = src[g, o2, o1, 0]
                dv_f32[at, :] = src[g, o2, o1, 1]

            for o1 in range(n):
                @pl.when(spot.rank(a=o1, b=o2)[1])
                def _():
                    if o1:
                        wait_bytes(ret2.at[g, o2, o1], r2_recv.at[g, o2, o1])
                        return
                    pl.when(o2 == 0)(lambda: put(0, res))
                    pl.when(o2 > 0)(lambda: put(0, ret1))

            for o1 in range(1, n):
                @pl.when(spot.rank(a=o1, b=o2)[1])
                def _():
                    put(o1, ret2)

        return carry

    lax.fori_loop(0, n_chunks + max(STORE_LAG, SUM_LAG + 2), step, 0)

    for g in range(GROUPS):
        for mine in (False, True):
            @pl.when(holds[g] if mine else jnp.logical_not(holds[g]))
            def _():
                wait_bytes(dq_got.at[pl.ds(0, heads - mine)], dq_recv.at[g])

    def put_dq(h, carry):
        dq_f32[pl.ds(h, q_local, stride=n_heads), :] = dq_got[h].astype(F32)
        return carry

    lax.fori_loop(0, n_heads, put_dq, 0)
    dq_bf[...] = dq_f32[...].astype(BF16)

    for g, spot in enumerate(spots):
        for mine in (False, True):
            @pl.when(holds[g] if mine else jnp.logical_not(holds[g]))
            def _():
                wait_bytes(aux_src.at[g, pl.ds(0, heads - mine)], aux_send.at[g])
        wait_bytes(kv1.at[g, pl.ds(1, n - 1)], k1_send.at[g])
        wait_bytes(q1.at[g, pl.ds(1, n - 1)], q1_send.at[g])

        @pl.when(holds[g])
        def _():
            wait_bytes(qd.at[g, 0, pl.ds(0, n - 1)], ql_send.at[g])
            wait_bytes(aux.at[g, 0, pl.ds(0, n - 1)], al_send.at[g])
            wait_bytes(line_sum.at[g], ls_send.at[g])
            wait_bytes(dq_src.at[g, pl.ds(1, plane - 1)], dq_send.at[g])
            wait_bytes(res.at[g, 0, pl.ds(1, n - 1)], r2_send.at[g, 0])
            for d in range(1, n):
                wait_bytes(res.at[g, d], r1_send.at[g, d])

        for d in range(1, n):
            @pl.when(spot.rank(b=d)[1])
            def _():
                wait_bytes(kv2.at[g, d], k2_send.at[g, d])
                wait_bytes(q1.at[g, d], q2_send.at[g, d])
                wait_bytes(res.at[g, d, pl.ds(1, n - 1)], r2_send.at[g, d])


def write_out(*refs):
    count = len(refs) // 2
    copies = [pltpu.make_async_copy(refs[k], refs[count + k], refs[-1].at[k]) for k in range(count)]
    for copy in copies:
        copy.start()
    for copy in copies:
        copy.wait()


def solution(mesh):
    cp_size = mesh.shape["cp"]
    n = {128: 4, 16: 2}[cp_size]
    spec_q = P(None, "cp", "heads", None)
    spec_kv = P("cp", "heads", None)
    spec_lse = P(None, "cp", "heads")

    def per_device(queries, key_vecs, value_vecs, attn_out, log_sum_exp, grad_out):
        _, q_local, n_heads, dim = queries.shape
        key_local = key_vecs.shape[0]
        prefix0 = (key_local - q_local) * cp_size
        plane, block = n * n, n * n * q_local
        q_rows, k_rows = q_local * n_heads, key_local * n_heads
        unit_rows = min(8, plane)
        dma = pltpu.SemaphoreType.DMA
        g4 = GROUPS
        vmem = pltpu.VMEM
        scratch = [
            vmem((q_rows, dim), F32), vmem((q_rows, dim), F32), vmem((k_rows, dim), F32), vmem((k_rows, dim), F32),
            vmem((128, 128), F32), vmem((2, n_heads, 128), F32),
            vmem((g4, n, n, 2, q_local, dim), BF16), vmem((g4, plane, 2, 128), F32), vmem((g4, n, n, 2, key_local, dim), BF16),
            vmem((g4, n, n, 2, q_local, dim), BF16),
            vmem((g4, 2, n, n, n, 2, q_local, dim), BF16), vmem((g4, 2, n, n, n, 2, 128), F32),
            vmem((g4, 2, n, plane // unit_rows, 2, 128), F32),
            vmem((g4, n, n, 2, key_local, dim), BF16), vmem((g4, n, n, 2, key_local, dim), BF16), vmem((n * key_local, 128), jnp.int32),
            vmem((g4, n, n, 2, key_local, dim), F32), vmem((g4, n, n, 2, key_local, dim), F32), vmem((g4, n, n, 2, key_local, dim), F32),
            vmem((g4, 2, n, dim, block), F32), vmem((g4, n, dim, block), F32), vmem((g4, n - 1, dim, block), F32),
            vmem((g4, plane, q_local, dim), BF16), vmem((n_heads, q_local, dim), BF16),
            vmem((q_rows, dim), F32),
            vmem((n * key_local, 2 * n * block), BF16), vmem((n * key_local, 2 * n * block), BF16),
            dma((g4,)), dma((g4,)), dma((g4, n)), dma((g4,)), dma((g4,)), dma((g4,)), dma((g4,)), dma((g4,)), dma((g4,)), dma((g4,)), dma((2, g4)), dma((2, g4)),
            dma((g4,)), dma((g4,)),
            dma((g4, n)), dma((g4, n)), dma((g4, n)), dma((g4, n)), dma((g4, n)), dma((g4, n, n)), dma((g4,)), dma((g4,)), dma((g4,)), dma((g4,)), dma((g4,)), dma((g4,)),
        ]
        anywhere = pl.BlockSpec(memory_space=pl.ANY)
        shapes = (jax.ShapeDtypeStruct((q_rows, dim), BF16), jax.ShapeDtypeStruct((k_rows, dim), F32), jax.ShapeDtypeStruct((k_rows, dim), F32))
        inside = pl.BlockSpec(memory_space=pltpu.VMEM)
        results = pl.pallas_call(
            functools.partial(kernel, n, prefix0, dim ** -0.5, n_heads),
            name="exchange_and_backward",
            out_shape=shapes,
            in_specs=[inside] * 6,
            out_specs=[inside] * 3,
            scratch_shapes=scratch,
            compiler_params=pltpu.CompilerParams(has_side_effects=True, collective_id=0, vmem_limit_bytes=VMEM_MIB * 1024 * 1024),
        )(queries.reshape(q_rows, dim), key_vecs.reshape(k_rows, dim), value_vecs.reshape(k_rows, dim), attn_out.reshape(q_rows, dim),
          log_sum_exp[0], grad_out.reshape(q_rows, dim))
        dq, dk, dv = pl.pallas_call(
            write_out,
            name="write_out",
            out_shape=shapes,
            in_specs=[inside] * 3,
            out_specs=[anywhere] * 3,
            scratch_shapes=[dma((3,))],
            compiler_params=pltpu.CompilerParams(vmem_limit_bytes=8 * 1024 * 1024),
        )(*results)
        return dq.reshape(queries.shape), dk.reshape(key_vecs.shape), dv.reshape(value_vecs.shape)

    return jax.shard_map(per_device, mesh=mesh, in_specs=(spec_q, spec_kv, spec_kv, spec_q, spec_lse, spec_q), out_specs=(spec_q, spec_kv, spec_kv), check_vma=False)
```

```python
import functools

import jax
import jax.numpy as jnp
from jax import lax
from jax.experimental import pallas as pl
from jax.experimental.pallas import tpu as pltpu
from jax.sharding import PartitionSpec as P

MESH = pl.DeviceIdType.MESH
GROUPS = 4
LINE_AXIS, FIRST_AXIS, SECOND_AXIS = zip((2, 1, 0), (0, 1, 2), (1, 0, 2), (1, 2, 0))
CHUNKS = ((0, 3), (0, 1), (1, 2), (2, 0), (2, 2), (0, 2), (0, 0), (3, 2), (2, 3), (3, 0), (3, 3), (3, 1), (2, 1), (1, 3), (1, 0), (1, 1))
BEFORE = (("k1", 0), ("q1", 0), ("k1", 1), ("q2", 0), ("q2", 2), ("q2", 3), ("k1", 2), ("q1", 1), ("q2", 1), ("line", 0), ("line", 1), ("k2", 0),
          ("line", 2), ("q1", 3), ("line", 3), ("k1", 3), ("line2", 0), ("line2", 2), ("line2", 1), ("q1", 2), ("k2", 1), ("k2", 2), ("k2", 3))
AFTER = {0: (("line2", 3),)}
LOG2E = 1.4426950408889634
FORWARD_LAG = 6
RELAY_LAG = 3
SUM_LAG = 14
STORE_LAG = 20
VMEM_MIB = 46
F32, BF16 = jnp.float32, jnp.bfloat16


def pick(table, g):
    if isinstance(g, int):
        return table[g]
    return (sum(v << (4 * k) for k, v in enumerate(table)) >> (4 * g)) & 15


def rank_at(n, a, b):
    if n == 2:
        rank = (a * 2 + b + 3) & 3
        return rank, rank < 3
    block = a >> 1
    rank = (((a & 1) << 2) + b + 7 - 2 * block) & 7
    return block * 7 + rank, rank < 7


class Spot:
    def __init__(self, n, chip, core, g):
        bits = n // 2
        self.n, self.chip, self.core = n, chip, core
        self.s_line, self.s_a, self.s_b = (pick([(2 - axis) * bits for axis in table], g) for table in (LINE_AXIS, FIRST_AXIS, SECOND_AXIS))
        self.line, self.a, self.b = ((chip >> s) & (n - 1) for s in (self.s_line, self.s_a, self.s_b))

    def turn(self, c, d):
        return (c + d) & (self.n - 1)

    def at(self, a=0, b=0, line=0):
        chip = self.chip
        for c, d, s in ((self.a, a, self.s_a), (self.b, b, self.s_b), (self.line, line, self.s_line)):
            if not (isinstance(d, int) and d == 0):
                chip = chip + ((self.turn(c, d) - c) << s)
        return chip

    def device(self, a=0, b=0, line=0):
        return (0, self.at(a, b, line) * 2 + self.core)

    def rank(self, a=0, b=0):
        return rank_at(self.n, self.turn(self.a, a), self.turn(self.b, b))


def kernel(n, prefix0, scale, n_heads, q_in, k_in, v_in, o_in, lse_in, do_in, dq_bf, dk_f32, dv_f32,
           q_raw, k_raw, v_raw, o_raw, lse_raw, do_raw, q_f32, do_f32, k_f32, v_f32, lse_pad, aux_rows,
           q_src, aux_src, kv_src, q1, qd, aux, rows, kv1, kv2, kpos_buf, res, ret1, ret2, dqt, part, line_half, line_sum, dq_src, dq_got,
           dq_f32, p_buf, ds_buf,
           in_sem, q1_send, q1_recv, q2_send, q2_recv, aux_send, aux_recv, ql_send, ql_recv, ql2_send, ql2_recv, al_send, al_recv, pair_send, pair_recv, k1_send, k1_recv,
           k2_send, k2_recv, r1_send, r1_recv, r2_send, r2_recv, part_send, part_recv, lh_send, lh_recv, ls_send, ls_recv, dq_send, dq_recv):
    me = lax.axis_index("cp")
    chip, core = me >> 1, me & 1
    bits = n // 2
    partner = (0, chip * 2 + 1 - core)
    spots = [Spot(n, chip, core, g) for g in range(GROUPS)]
    holds = [s.rank()[1] for s in spots]
    heads = n_heads // GROUPS
    q_local, key_local = q_src.shape[4], kv_src.shape[4]
    plane = n * n
    unit_rows = min(8, plane)
    width = unit_rows * q_local
    block = plane * q_local
    n_rows = block // width
    keys_in = n * key_local

    def remote(src, dst, send, recv, device):
        return pltpu.make_async_remote_copy(src, dst, send, recv, device_id=device, device_id_type=MESH)

    def wait_bytes(ref, sem):
        pltpu.make_async_copy(ref, ref, sem).wait()

    loads = [pltpu.make_async_copy(a, b, in_sem.at[k]) for k, (a, b) in enumerate(
        [(q_in, q_raw), (do_in, do_raw), (o_in, o_raw), (lse_in, lse_raw), (k_in, k_raw), (v_in, v_raw)])]
    for copy in loads:
        copy.start()

    barrier = pltpu.get_barrier_semaphore()
    met = 1
    pl.semaphore_signal(barrier, inc=1, device_id=partner, device_id_type=MESH)
    for s_a, s_b in ((2 * bits, bits), (bits, 0), (0, 2 * bits)):
        c_a, c_b = (chip >> s_a) & (n - 1), (chip >> s_b) & (n - 1)
        for a in range(n):
            for b in range(1, n):
                there = chip + ((((c_a + a) & (n - 1)) - c_a) << s_a) + ((((c_b + b) & (n - 1)) - c_b) << s_b)
                pl.semaphore_signal(barrier, inc=1, device_id=(0, there * 2 + core), device_id_type=MESH)
                met += 1

    def widen(src, dst, count):
        per = n_heads * 4

        def go(t, carry):
            at = pl.ds(pl.multiple_of(t * per, 8), per)
            dst[at] = src[at].astype(F32)
            return carry

        lax.fori_loop(0, count // 4, go, 0)

    order = [g for name, g in BEFORE if name == "q1"]
    for copy in loads[:2]:
        copy.wait()
    widen(q_raw, q_f32, q_local)
    widen(do_raw, do_f32, q_local)
    for g in order:
        spot = spots[g]

        def lay_out_q(u, carry):
            rank, _ = spot.rank(u >> bits, u & (n - 1))
            h = g * heads + jnp.minimum(rank, heads - 1)
            q_src[g, u >> bits, u & (n - 1), 0] = q_f32[pl.ds(h, q_local, stride=n_heads), :].astype(BF16)
            q_src[g, u >> bits, u & (n - 1), 1] = do_f32[pl.ds(h, q_local, stride=n_heads), :].astype(BF16)
            return carry

        lax.fori_loop(0, plane, lay_out_q, 0, unroll=8)
    pl.semaphore_wait(barrier, met)

    def q_first(g):
        spot = spots[g]
        for d in range(1, n):
            remote(q_src.at[g, d], q1.at[g, d], q1_send, q1_recv.at[g], spot.device(a=d)).start()

    def aux_out(g):
        spot = spots[g]
        for u in range(1, plane):
            d1, d2 = u >> bits, u & (n - 1)

            @pl.when(spot.rank(d1, d2)[1])
            def _():
                remote(aux_src.at[g, u], aux.at[g, 0, spot.line, spot.b, spot.a], aux_send.at[g], aux_recv.at[g], spot.device(d1, d2)).start()

    def q_second(g):
        spot = spots[g]
        wait_bytes(q1.at[g, pl.ds(1, n - 1)], q1_recv.at[g])

        @pl.when(holds[g])
        def _():
            for o1 in range(n):
                qd[g, 0, spot.line, spot.b, spot.turn(spot.a, -o1)] = q1[g, o1, 0] if o1 else q_src[g, 0, 0]
            aux[g, 0, spot.line, spot.b, spot.a] = aux_src[g, 0]

        for d in range(1, n):
            @pl.when(spot.rank(b=d)[1])
            def _():
                there = spot.device(b=d)
                for o1 in range(n):
                    src = q1.at[g, o1, d] if o1 else q_src.at[g, 0, d]
                    remote(src, qd.at[g, 0, spot.line, spot.b, spot.turn(spot.a, -o1)], q2_send.at[g], q2_recv.at[g], there).start()

    def k_first(g):
        for d in range(1, n):
            remote(kv_src.at[g, d], kv1.at[g, d], k1_send, k1_recv.at[g], spots[g].device(a=d)).start()

    def k_second(g, own):
        for d in range(1, n):
            @pl.when(spots[g].rank(b=d)[1])
            def _():
                there = spots[g].device(b=d)
                if own:
                    remote(kv_src.at[g, 0, d], kv2.at[g, d, 0], k2_send.at[g], k2_recv.at[g, d - 1], there).start()
                else:
                    remote(kv1.at[g, pl.ds(1, n - 1), d], kv2.at[g, d, pl.ds(1, n - 1)], k2_send.at[g], k2_recv.at[g, d - 1], there).start()

    beside = (1, n - 1) if n == 4 else (1,)
    n_half = n // 2

    def q_line(g):
        spot = spots[g]
        for d in beside:
            remote(qd.at[g, 0, spot.line], qd.at[g, 0, spot.line], ql_send.at[g], ql_recv.at[g], spot.device(line=d)).start()
        for d in range(1, n):
            remote(aux.at[g, 0, spot.line], aux.at[g, 0, spot.line], al_send.at[g], al_recv.at[g], spot.device(line=d)).start()

    def line_on(g):
        spot = spots[g]
        if n == 4:
            @pl.when(holds[g])
            def _():
                wait_bytes(qd.at[g, 0, pl.ds(0, 2)], ql_recv.at[g])
                for k, (d, there) in enumerate(((n - 1, 1), (1, n - 1))):
                    piece = qd.at[g, 0, spot.turn(spot.line, d), pl.ds(k * n_half, n_half)]
                    remote(piece, piece, ql2_send.at[g], ql2_recv.at[g], spot.device(line=there)).start()

    def line_out(g):
        @pl.when(holds[g])
        def _():
            wait_bytes(q_src.at[g, pl.ds(1, n - 1)], q2_recv.at[g])
            wait_bytes(aux_src.at[g, pl.ds(1, plane - 1)], aux_recv.at[g])
            q_line(g)

    def pass_on(g):
        wait_bytes(kv1.at[g, pl.ds(1, n - 1)], k1_recv.at[g])
        k_second(g, False)

    def keys_out(g):
        k_first(g)
        k_second(g, True)

    def pair_copies(g):
        return (remote(qd.at[g, 0], qd.at[g, 1], pair_send.at[0, g], pair_recv.at[0, g], partner),
                remote(aux.at[g, 0], aux.at[g, 1], pair_send.at[1, g], pair_recv.at[1, g], partner))

    def share_queries(g):
        wait_bytes(qd.at[g, 0, 0], ql2_recv.at[g] if n == 4 else ql_recv.at[g])
        wait_bytes(aux.at[g, 0, pl.ds(0, n - 1)], al_recv.at[g])
        for copy in pair_copies(g):
            copy.start()

    acts = {"q1": q_first, "q2": q_second, "k1": keys_out, "k2": pass_on, "line": line_out, "line2": line_on}
    chunks = [(g, o2) for g, o2 in CHUNKS if o2 < n]
    n_chunks = len(chunks)
    first = [min(k for k, c in enumerate(chunks) if c[0] == g) for g in range(GROUPS)]
    last = [max(k for k, c in enumerate(chunks) if c[0] == g) for g in range(GROUPS)]
    after = {k: list(v) for k, v in AFTER.items()} if n == 4 else {-1: [a for v in AFTER.values() for a in v]}
    lined = {g: k for k, v in after.items() for name, g in v if name == "line2"}
    before = list(BEFORE) + after.pop(-1, [])
    for g in order:
        q_first(g)
    for copy in loads[2:4]:
        copy.wait()
    lse_pad[0:q_local, 0:n_heads] = lse_raw[...]
    lse_t = lse_pad[...].T[0:n_heads]
    head_group = lax.div(lax.broadcasted_iota(jnp.int32, (n_heads, 128), 0), heads)
    lane = lax.broadcasted_iota(jnp.int32, (n_heads, 128), 1)
    base = jnp.zeros((n_heads, 128), jnp.int32)
    for g, spot in enumerate(spots):
        base = jnp.where(head_group == g, ((spot.b * n + spot.a) & (unit_rows - 1)) * q_local, base)
    row_lse, row_delta = jnp.zeros((n_heads, 128), F32), jnp.zeros((n_heads, 128), F32)
    for t in range(q_local):
        at = pl.ds(t * n_heads, n_heads)
        delta = jnp.sum(do_f32[at] * o_raw[at].astype(F32), axis=1, keepdims=True)
        row_delta = jnp.where(lane == base + t, delta, row_delta)
        row_lse = jnp.where(lane == base + t, lse_t[:, t:t + 1], row_lse)
    aux_rows[0] = row_lse
    aux_rows[1] = row_delta
    for g in order:
        spot = spots[g]

        def lay_out_aux(u, carry):
            rank, _ = spot.rank(u >> bits, u & (n - 1))
            h = g * heads + jnp.minimum(rank, heads - 1)
            aux_src[g, u, 0:1] = aux_rows[0, pl.ds(h, 1), :]
            aux_src[g, u, 1:2] = aux_rows[1, pl.ds(h, 1), :]
            return carry

        lax.fori_loop(0, plane, lay_out_aux, 0, unroll=8)
    for g in order:
        aux_out(g)
    for copy in loads[4:]:
        copy.wait()
    widen(k_raw, k_f32, key_local)
    widen(v_raw, v_f32, key_local)
    for g in [g for name, g in before if name == "k1"]:
        spot = spots[g]

        def lay_out_kv(u, carry):
            rank, _ = spot.rank(u >> bits, u & (n - 1))
            h = g * heads + jnp.minimum(rank, heads - 1)
            kv_src[g, u >> bits, u & (n - 1), 0] = k_f32[pl.ds(h, key_local, stride=n_heads), :].astype(BF16)
            kv_src[g, u >> bits, u & (n - 1), 1] = v_f32[pl.ds(h, key_local, stride=n_heads), :].astype(BF16)
            return carry

        lax.fori_loop(0, plane, lay_out_kv, 0, unroll=4)
    for name, g in before:
        if name != "q1":
            acts[name](g)
    shares = {g: max(first[g] - 2, lined.get(g, -1), -1) for g in range(GROUPS)}

    def share(g):
        pl.when(holds[g])(lambda: share_queries(g))

    for g in range(GROUPS):
        if shares[g] < 0:
            share(g)
    codes = [sum((g * 4 + o2) << (4 * k) for k, (g, o2) in enumerate(chunks[w:w + 8])) for w in range(0, n_chunks, 8)]
    codes = [c - (1 << 32) if c >= 1 << 31 else c for c in codes]
    begins = sum(1 << k for k in first)

    def chunk_of(i):
        word = codes[0] if len(codes) == 1 else jnp.where(i < 8, codes[0], codes[1])
        code = word >> (4 * (i & 7))
        return (code >> 2) & 3, code & 3

    def compute(i):
        g, o2 = chunk_of(i)
        spot = Spot(n, chip, core, g)

        @pl.when(((begins >> i) & 1) == 1)
        def _():
            for copy in pair_copies(g):
                copy.wait()
            for half in range(2):
                for l in range(n):
                    units = aux[g, half, l].reshape(n_rows, unit_rows, 2, 128)
                    rows[g, half, l] = jnp.sum(units, axis=1)
            dqt[g] = jnp.zeros(dqt.shape[1:], F32)

        @pl.when(o2 == 0)
        def _():
            kv2[g, 0, 0] = kv_src[g, 0, 0]
            for o1 in range(1, n):
                kv2[g, 0, o1] = kv1[g, o1, 0]

        @pl.when(o2 > 0)
        def _():
            wait_bytes(kv2.at[g, o2], k2_recv.at[g, o2 - 1])

        for o1 in range(n):
            first = (spot.at(a=-o1, b=-o2) * 2 + core) * key_local - prefix0
            kpos_buf[pl.ds(o1 * key_local, key_local)] = first + lax.broadcasted_iota(jnp.int32, (key_local, 128), 0)
        keys = kv2[g, o2, :, 0].reshape(keys_in, 128)
        values = kv2[g, o2, :, 1].reshape(keys_in, 128)
        keys_t = keys.T

        def q_step(s, carry):
            half = s & 1
            l = spot.turn(spot.line, 1 + (s >> 1))
            q = qd[g, half, l, :, :, 0].reshape(block, 128)
            do = qd[g, half, l, :, :, 1].reshape(block, 128)
            lse2 = jnp.concatenate([rows[g, half, l, r, 0:1, 0:width] for r in range(n_rows)], axis=1) * LOG2E
            delta = jnp.concatenate([rows[g, half, l, r, 1:2, 0:width] for r in range(n_rows)], axis=1)
            lanes = lax.broadcasted_iota(jnp.int32, (1, block), 1)
            unit = lax.div(lanes, q_local)
            q_chip = (l << spot.s_line) + (lax.div(unit, n) << spot.s_b) + (lax.rem(unit, n) << spot.s_a)
            qpos = (q_chip * 2 + ((core + half) & 1)) * q_local + lax.rem(lanes, q_local)
            kpos = jnp.concatenate([kpos_buf[...]] * n_rows, axis=1)[:, 0:block]
            s_ = lax.dot_general(keys, q, (((1,), (1,)), ((), ())), preferred_element_type=F32)
            p = jnp.where(kpos <= qpos, jnp.exp2(s_ * (scale * LOG2E) - lse2), 0.0)
            dp = lax.dot_general(values, do, (((1,), (1,)), ((), ())), preferred_element_type=F32)
            ds = (p * (dp - delta)).astype(BF16)
            at = pl.ds(pl.multiple_of((half * n + l) * block, block), block)
            p_buf[:, at] = p.astype(BF16)
            ds_buf[:, at] = ds
            return carry

        lax.fori_loop(0, 2 * n, q_step, 0, unroll=8)
        q_all = qd[g, :, :, :, :, 0].reshape(2 * n * block, 128)
        do_all = qd[g, :, :, :, :, 1].reshape(2 * n * block, 128)
        for half in range(2):
            for l in range(n):
                at = pl.ds((half * n + l) * block, block)
                dqt[g, half, l] += jnp.dot(keys_t, ds_buf[:, at], preferred_element_type=F32)
        res[g, o2, :, 0] = (jnp.dot(ds_buf[...], q_all, preferred_element_type=F32) * scale).reshape(n, key_local, 128)
        res[g, o2, :, 1] = jnp.dot(p_buf[...], do_all, preferred_element_type=F32).reshape(n, key_local, 128)

    def part_copy(g):
        return remote(dqt.at[g, 1], part.at[g], part_send.at[g], part_recv.at[g], partner)

    def half_out(g, spot):
        if n == 4:
            for k, d in enumerate(beside):
                src = dqt.at[g, 0, spot.turn(spot.line, 2), pl.ds(k * 64, 64)]
                remote(src, line_half.at[g, k], lh_send.at[g], lh_recv.at[g], spot.device(line=d)).start()

    def line_sum_out(g, spot):
        if n == 4:
            wait_bytes(line_half.at[g], lh_recv.at[g])
            for k, d in enumerate(beside):
                l = spot.turn(spot.line, d)
                dqt[g, 0, l, k * 64:k * 64 + 64] = dqt[g, 0, l, k * 64:k * 64 + 64] + line_half[g, k]
        for k, d in enumerate(beside):
            remote(dqt.at[g, 0, spot.turn(spot.line, d)], line_sum.at[g, k], ls_send.at[g], ls_recv.at[g], spot.device(line=d)).start()

    def dq_copy(g, spot, u):
        b, a = spot.turn(spot.b, u >> bits), spot.turn(spot.a, u & (n - 1))
        h = g * heads + jnp.minimum(spot.rank()[0], heads - 1)
        return remote(dq_src.at[g, b * n + a], dq_got.at[h], dq_send.at[g], dq_recv.at[g], spot.device(a=u & (n - 1), b=u >> bits))

    def first_back(g, o2, spot):
        return remote(res.at[g, o2], ret1.at[g, o2], r1_send.at[g], r1_recv.at[g, o2 - 1], spot.device(b=-o2))

    def second_back(g, o2, o1, spot, src):
        return remote(src.at[g, o2, o1], ret2.at[g, o2, o1], r2_send.at[g], r2_recv.at[g, o2], spot.device(a=-o1))

    def step(i, carry):
        @pl.when(i < n_chunks)
        def _():
            g, o2 = chunk_of(i)
            spot = Spot(n, chip, core, g)

            @pl.when(spot.rank()[1])
            def _():
                compute(i)

                @pl.when(o2 > 0)
                def _():
                    first_back(g, o2, spot).start()

                @pl.when(o2 == 0)
                def _():
                    for o1 in range(1, n):
                        second_back(g, 0, o1, spot, res).start()

        for k, todo in after.items():
            @pl.when(i == k)
            def _():
                for name, g in todo:
                    acts[name](g)

        for g, spot in enumerate(spots):
            @pl.when(jnp.logical_and(i == last[g], holds[g]))
            def _():
                part_copy(g).start()

            @pl.when(jnp.logical_and(i == last[g] + 1, holds[g]))
            def _():
                part_copy(g).wait()
                for d in ((2, 1, 3, 0) if n == 4 else (1, 0)):
                    l = spot.turn(spot.line, d)
                    dqt[g, 0, l] = dqt[g, 0, l] + part[g, l]
                half_out(g, spot)

            @pl.when(jnp.logical_and(i == last[g] + 1 + RELAY_LAG, holds[g]))
            def _():
                line_sum_out(g, spot)

            @pl.when(jnp.logical_and(i == last[g] + 1 + SUM_LAG, holds[g]))
            def _():
                wait_bytes(line_sum.at[g], ls_recv.at[g])
                total = dqt[g, 0, spot.line]
                for d in range(len(beside)):
                    total = total + line_sum[g, d]
                dq_src[g] = (total * scale).T.astype(BF16).reshape(plane, q_local, 128)
                h = g * heads + spot.rank()[0]
                dq_got[h] = dq_src[g, spot.b * n + spot.a]

                def go(u, carry):
                    dq_copy(g, spot, u).start()
                    return carry

                lax.fori_loop(1, plane, go, 0)

            if shares[g] >= 0:
                @pl.when(i == shares[g])
                def _():
                    share(g)

        j = i - FORWARD_LAG

        @pl.when(jnp.logical_and(j >= 0, j < n_chunks))
        def _():
            g, o2 = chunk_of(j)
            spot = Spot(n, chip, core, g)

            @pl.when(jnp.logical_and(o2 > 0, spot.rank(b=o2)[1]))
            def _():
                wait_bytes(ret1.at[g, o2], r1_recv.at[g, o2 - 1])
                for o1 in range(1, n):
                    second_back(g, o2, o1, spot, ret1).start()

        k = i - STORE_LAG

        @pl.when(jnp.logical_and(k >= 0, k < n_chunks))
        def _():
            g, o2 = chunk_of(k)
            spot = Spot(n, chip, core, g)

            def put(o1, src):
                rank, _ = spot.rank(a=o1, b=o2)
                at = pl.ds(g * heads + rank, key_local, stride=n_heads)
                dk_f32[at, :] = src[g, o2, o1, 0]
                dv_f32[at, :] = src[g, o2, o1, 1]

            @pl.when(spot.rank(b=o2)[1])
            def _():
                pl.when(o2 == 0)(lambda: put(0, res))
                pl.when(o2 > 0)(lambda: put(0, ret1))

            column = spot.turn(spot.b, o2)
            short = jnp.logical_and((column & 1) == 0, column != spot.a)
            for less in range(2):
                if n - 1 > less:
                    @pl.when(short if less else jnp.logical_not(short))
                    def _():
                        wait_bytes(ret2.at[g, o2, pl.ds(1, n - 1 - less)], r2_recv.at[g, o2])

            for o1 in range(1, n):
                @pl.when(spot.rank(a=o1, b=o2)[1])
                def _():
                    put(o1, ret2)

        return carry

    lax.fori_loop(0, n_chunks + max(STORE_LAG, SUM_LAG + 2), step, 0)

    for g in range(GROUPS):
        for mine in (False, True):
            @pl.when(holds[g] if mine else jnp.logical_not(holds[g]))
            def _():
                wait_bytes(dq_got.at[pl.ds(0, heads - mine)], dq_recv.at[g])

    def put_dq(h, carry):
        dq_f32[pl.ds(h, q_local, stride=n_heads), :] = dq_got[h].astype(F32)
        return carry

    lax.fori_loop(0, n_heads, put_dq, 0)
    dq_bf[...] = dq_f32[...].astype(BF16)

    wait_bytes(q1.at[pl.ds(0, GROUPS), pl.ds(1, n - 1)], q1_send)
    wait_bytes(kv1.at[pl.ds(0, GROUPS), pl.ds(1, n - 1)], k1_send)
    for g, spot in enumerate(spots):
        even = (spot.a & 1) == 0
        for mine in (False, True):
            @pl.when(holds[g] if mine else jnp.logical_not(holds[g]))
            def _():
                wait_bytes(aux_src.at[g, pl.ds(0, heads - mine)], aux_send.at[g])
        short = jnp.logical_and(even, holds[g])
        for less in range(2):
            if n - 1 > less:
                @pl.when(short if less else jnp.logical_not(short))
                def _():
                    wait_bytes(q1.at[g, pl.ds(0, n - 1 - less)], q2_send.at[g])
                    wait_bytes(kv2.at[g, pl.ds(0, n - 1 - less)], k2_send.at[g])

            @pl.when(even if less else jnp.logical_not(even))
            def _():
                wait_bytes(ret2.at[g, pl.ds(0, n - less), pl.ds(1, n - 1)], r2_send.at[g])

        @pl.when(holds[g])
        def _():
            wait_bytes(qd.at[g, 0, pl.ds(0, len(beside))], ql_send.at[g])
            wait_bytes(aux.at[g, 0, pl.ds(0, n - 1)], al_send.at[g])
            wait_bytes(line_sum.at[g], ls_send.at[g])
            wait_bytes(dq_src.at[g, pl.ds(1, plane - 1)], dq_send.at[g])
            wait_bytes(ret1.at[g, pl.ds(0, n - 1)], r1_send.at[g])
            if n == 4:
                wait_bytes(qd.at[g, 0, 0], ql2_send.at[g])
                wait_bytes(line_half.at[g], lh_send.at[g])


def write_out(*refs):
    count = len(refs) // 2
    copies = [pltpu.make_async_copy(refs[k], refs[count + k], refs[-1].at[k]) for k in range(count)]
    for copy in copies:
        copy.start()
    for copy in copies:
        copy.wait()


def solution(mesh):
    cp_size = mesh.shape["cp"]
    n = {128: 4, 16: 2}[cp_size]
    spec_q = P(None, "cp", "heads", None)
    spec_kv = P("cp", "heads", None)
    spec_lse = P(None, "cp", "heads")

    def per_device(queries, key_vecs, value_vecs, attn_out, log_sum_exp, grad_out):
        _, q_local, n_heads, dim = queries.shape
        key_local = key_vecs.shape[0]
        prefix0 = (key_local - q_local) * cp_size
        plane, block = n * n, n * n * q_local
        q_rows, k_rows = q_local * n_heads, key_local * n_heads
        unit_rows = min(8, plane)
        dma = pltpu.SemaphoreType.DMA
        g4 = GROUPS
        vmem = pltpu.VMEM
        scratch = [
            vmem((q_rows, dim), BF16), vmem((k_rows, dim), BF16), vmem((k_rows, dim), BF16), vmem((q_rows, dim), BF16),
            vmem((q_local, n_heads), F32), vmem((q_rows, dim), BF16),
            vmem((q_rows, dim), F32), vmem((q_rows, dim), F32), vmem((k_rows, dim), F32), vmem((k_rows, dim), F32),
            vmem((128, 128), F32), vmem((2, n_heads, 128), F32),
            vmem((g4, n, n, 2, q_local, dim), BF16), vmem((g4, plane, 2, 128), F32), vmem((g4, n, n, 2, key_local, dim), BF16),
            vmem((g4, n, n, 2, q_local, dim), BF16),
            vmem((g4, 2, n, n, n, 2, q_local, dim), BF16), vmem((g4, 2, n, n, n, 2, 128), F32),
            vmem((g4, 2, n, plane // unit_rows, 2, 128), F32),
            vmem((g4, n, n, 2, key_local, dim), BF16), vmem((g4, n, n, 2, key_local, dim), BF16), vmem((n * key_local, 128), jnp.int32),
            vmem((g4, n, n, 2, key_local, dim), F32), vmem((g4, n, n, 2, key_local, dim), F32), vmem((g4, n, n, 2, key_local, dim), F32),
            vmem((g4, 2, n, dim, block), F32), vmem((g4, n, dim, block), F32), vmem((g4, 2, dim // 2, block), F32), vmem((g4, n // 2, dim, block), F32),
            vmem((g4, plane, q_local, dim), BF16), vmem((n_heads, q_local, dim), BF16),
            vmem((q_rows, dim), F32),
            vmem((n * key_local, 2 * n * block), BF16), vmem((n * key_local, 2 * n * block), BF16),
            dma((6,)), dma, dma((g4,)), dma((g4,)), dma((g4,)), dma((g4,)), dma((g4,)), dma((g4,)), dma((g4,)), dma((g4,)), dma((g4,)),
            dma((g4,)), dma((g4,)), dma((2, g4)), dma((2, g4)), dma, dma((g4,)), dma((g4,)), dma((g4, n - 1)), dma((g4,)), dma((g4, n - 1)),
            dma((g4,)), dma((g4, n)), dma((g4,)), dma((g4,)), dma((g4,)), dma((g4,)), dma((g4,)), dma((g4,)), dma((g4,)), dma((g4,)),
        ]
        anywhere = pl.BlockSpec(memory_space=pl.ANY)
        shapes = (jax.ShapeDtypeStruct((q_rows, dim), BF16), jax.ShapeDtypeStruct((k_rows, dim), F32), jax.ShapeDtypeStruct((k_rows, dim), F32))
        inside = pl.BlockSpec(memory_space=pltpu.VMEM)
        operands = (queries.reshape(q_rows, dim), key_vecs.reshape(k_rows, dim), value_vecs.reshape(k_rows, dim), attn_out.reshape(q_rows, dim),
                    log_sum_exp[0], grad_out.reshape(q_rows, dim))
        results = pl.pallas_call(
            functools.partial(kernel, n, prefix0, dim ** -0.5, n_heads),
            name="exchange_and_backward",
            out_shape=shapes,
            in_specs=[anywhere] * 6,
            out_specs=[inside] * 3,
            scratch_shapes=scratch,
            compiler_params=pltpu.CompilerParams(has_side_effects=True, collective_id=0, vmem_limit_bytes=VMEM_MIB * 1024 * 1024),
        )(*(pltpu.with_memory_space_constraint(x, pltpu.HBM) for x in operands))
        dq, dk, dv = pl.pallas_call(
            write_out,
            name="write_out",
            out_shape=shapes,
            in_specs=[inside] * 3,
            out_specs=[anywhere] * 3,
            scratch_shapes=[dma((3,))],
            compiler_params=pltpu.CompilerParams(vmem_limit_bytes=8 * 1024 * 1024),
        )(*results)
        return dq.reshape(queries.shape), dk.reshape(key_vecs.shape), dv.reshape(value_vecs.shape)

    return jax.shard_map(per_device, mesh=mesh, in_specs=(spec_q, spec_kv, spec_kv, spec_q, spec_lse, spec_q), out_specs=(spec_q, spec_kv, spec_kv), check_vma=False)
```
